256 devices in a mesh: ang: 16 (over x, z_hi, core), tile: 16 (over y, z_lo).
Axes of the slice: x: 4, y: 4, z: 8 (z_hi: 2, z_lo: 4; z = z_hi * 4 + z_lo), core: 2. Of those that a mesh axis runs over, the one named last changes fastest.
Arguments:
- volume: float32 [256, 128, 256], P('ang', 'tile'), may hold values from -6 to 6
- phase: float32 [16, 128, 256], P('ang', 'tile'), may hold values from -6 to 6
- dual: float32 [16, 128, 256], P('ang', 'tile'), may hold values from -3 to 3
- probe_real: float32 [128, 128], replicated, may hold values from -4 to 4
- probe_imag: float32 [128, 128], replicated, may hold values from -4 to 4
- intensity: float32 [16, 64, 128, 128], P('ang', 'tile'), may hold values from 0.05 to 4
- offsets: int32 [16, 64], P('ang', 'tile'), may hold values from 0 to 128
- angle_index: int32 [16], P('ang'), may hold values from 0 to 180
Outputs:
- phase_new: float32 [16, 128, 256], P('ang', 'tile')
- volume_new: float32 [256, 128, 256], P('ang', 'tile')
- dual_new: float32 [16, 128, 256], P('ang', 'tile')
The draws below stay inside these ranges and needn't reach their ends.
Inputs may be any that keep to these rules, and one draw needn't show every extreme that they name: `offsets`: the probe's 128 columns starting at the offset lie inside the 256 columns of a projection.
All inputs are finite; a program needn't handle non-finite values.
Results may differ from the reference program's by a relative error of at most 0.015.
Values may be sent and summed in bfloat16 or wider, within the bound.
A program may use at most 64 MiB of HBM per device.

```python
import math
import jax
import jax.numpy as jnp
from jax import lax

N = 256
PROBE = 128
BAND = 128
POS = 64
ANG = 16


def plant(entries, key, least, largest):
    dims = entries.shape
    spot = [jax.random.randint(jax.random.fold_in(key, axis), (), 0, dims[axis]) for axis in range(len(dims))]
    entries = entries.at[tuple(spot)].set(least)
    longest = dims.index(max(dims))
    spot[longest] = (spot[longest] + 1) % dims[longest]
    return entries.at[tuple(spot)].set(largest)


def shard_levels(rng, dims, pieces, smallest, high):
    factor_of, own = 1.0, jax.random.fold_in(rng, 6)
    for dim, shards_of in pieces:
        draws = jnp.exp(jax.random.uniform(jax.random.fold_in(own, dim), (shards_of,), jnp.float32, smallest / len(pieces), high / len(pieces)))
        factor_of = factor_of * jnp.repeat(draws, dims[dim] // shards_of).reshape([-1 if axis == dim else 1 for axis in range(len(dims))])
    return factor_of


def normal_values(key, dims, deviation, most, shards=(), kind=jnp.bfloat16):
    array = deviation * jax.random.normal(key, dims, jnp.float32)
    if shards:
        array = array * shard_levels(key, dims, shards, -0.22, 0.18)
    return jnp.clip(array, -most, most).astype(kind)


def setup_inputs(seed: int = 0) -> dict:
    arg_keys = jax.random.split(jax.random.key(seed), 9)
    volume = normal_values(arg_keys[0], (N, BAND, N), 1.0, 6.0, ((0, 16), (1, 16)), jnp.float32)
    phase = normal_values(arg_keys[1], (ANG, BAND, N), 1.0, 6.0, ((0, 16), (1, 16)), jnp.float32)
    dual = normal_values(arg_keys[2], (ANG, BAND, N), 0.5, 3.0, ((0, 16), (1, 16)), jnp.float32)
    probe_real = normal_values(arg_keys[3], (PROBE, PROBE), 0.7, 4.0, (), jnp.float32)
    probe_imag = normal_values(arg_keys[4], (PROBE, PROBE), 0.7, 4.0, (), jnp.float32)
    intensity = jnp.clip(jnp.exp(math.log(4.0) - 4.3820266 * jax.random.uniform(arg_keys[5], (ANG, POS, PROBE, PROBE), jnp.float32) ** shard_levels(arg_keys[5], (ANG, POS, PROBE, PROBE), ((0, 16), (1, 16)), -0.2, 0.2)), 0.05, 4.0)
    offsets = plant(jax.random.randint(arg_keys[6], (ANG, POS), 0, N - PROBE + 1), jax.random.fold_in(arg_keys[6], 1), 0, N - PROBE).astype(jnp.int32)
    angle_index = plant(jax.random.randint(arg_keys[7], (ANG,), 0, 181), jax.random.fold_in(arg_keys[7], 1), 0, 180).astype(jnp.int32)
    return {"volume": volume, "phase": phase, "dual": dual, "probe_real": probe_real, "probe_imag": probe_imag, "intensity": intensity, "offsets": offsets, "angle_index": angle_index}


angle_center = 90.0
rho_weight = 1.0
eta_step = 0.01
tau_step = 1.0
smooth_weight = 0.25

def dft_tables(length):
    index = jnp.arange(length, dtype=jnp.int32)
    product = index[:, None] * index[None, :] % length
    phases = product.astype(jnp.float32) * (2.0 * math.pi / length)
    return (jnp.cos(phases), jnp.sin(phases))

def signed_freq(length):
    index = jnp.arange(length, dtype=jnp.int32)
    return jnp.where(index < length // 2, index, index - length).astype(jnp.float32)

def shear_coefficients(angle_number):
    theta = (angle_number.astype(jnp.float32) - angle_center) * (math.pi / 360.0)
    return (-jnp.tan(0.5 * theta), jnp.sin(theta))

def shear_last(volume_part, shifts, cos_half, sin_half, frequency):
    row_count, depth_count, length = volume_part.shape
    flattened = volume_part.reshape(row_count * depth_count, length)
    real_part = jnp.dot(flattened, cos_half, preferred_element_type=jnp.float32).reshape(row_count, depth_count, length)
    imag_part = -jnp.dot(flattened, sin_half, preferred_element_type=jnp.float32).reshape(row_count, depth_count, length)
    angles = 2.0 * math.pi / length * shifts[:, None] * frequency[None, :]
    cosine_turn = jnp.cos(angles)[:, None, :]
    sine_turn = jnp.sin(angles)[:, None, :]
    turned_r = (real_part * cosine_turn + imag_part * sine_turn).astype(jnp.bfloat16).reshape(row_count * depth_count, length)
    turned_i = (imag_part * cosine_turn - real_part * sine_turn).astype(jnp.bfloat16).reshape(row_count * depth_count, length)
    result = jnp.dot(turned_r, cos_half, preferred_element_type=jnp.float32) - jnp.dot(turned_i, sin_half, preferred_element_type=jnp.float32)
    return (result / length).reshape(row_count, depth_count, length)

def shear_first(volume_part, shifts, cos_half, sin_half, frequency):
    row_count, depth_count, length = volume_part.shape
    flattened = volume_part.reshape(row_count, depth_count * length)
    real_part = jnp.dot(cos_half, flattened, preferred_element_type=jnp.float32).reshape(row_count, depth_count, length)
    imag_part = -jnp.dot(sin_half, flattened, preferred_element_type=jnp.float32).reshape(row_count, depth_count, length)
    angles = 2.0 * math.pi / row_count * frequency[:, None] * shifts[None, :]
    cosine_turn = jnp.cos(angles)[:, None, :]
    sine_turn = jnp.sin(angles)[:, None, :]
    turned_r = (real_part * cosine_turn + imag_part * sine_turn).astype(jnp.bfloat16).reshape(row_count, depth_count * length)
    turned_i = (imag_part * cosine_turn - real_part * sine_turn).astype(jnp.bfloat16).reshape(row_count, depth_count * length)
    result = jnp.dot(cos_half, turned_r, preferred_element_type=jnp.float32) - jnp.dot(sin_half, turned_i, preferred_element_type=jnp.float32)
    return (result / row_count).reshape(row_count, depth_count, length)

def project_lines(volume_part, coef_a, cos_half, sin_half, cos_full, sin_full, frequency):
    row_count, depth_count, length = volume_part.shape
    flattened = volume_part.reshape(row_count * depth_count, length)
    real_part = jnp.dot(flattened, cos_half, preferred_element_type=jnp.float32).reshape(row_count, depth_count, length)
    imag_part = -jnp.dot(flattened, sin_half, preferred_element_type=jnp.float32).reshape(row_count, depth_count, length)
    centred = jnp.arange(row_count, dtype=jnp.int32).astype(jnp.float32) - 0.5 * row_count
    angles = 2.0 * math.pi / length * (coef_a * centred)[:, None] * frequency[None, :]
    cosine_turn = jnp.cos(angles)[:, None, :]
    sine_turn = jnp.sin(angles)[:, None, :]
    summed_r = lax.optimization_barrier(jnp.sum(real_part * cosine_turn + imag_part * sine_turn, axis=0))
    summed_i = lax.optimization_barrier(jnp.sum(imag_part * cosine_turn - real_part * sine_turn, axis=0))
    lines = jnp.dot(summed_r, cos_full, precision=lax.Precision.HIGHEST) - jnp.dot(summed_i, sin_full, precision=lax.Precision.HIGHEST)
    return lines / (length * math.sqrt(length))

def back_lines(lines, row_count, coef_a, cos_half, sin_half, cos_full, sin_full, frequency):
    depth_count, length = lines.shape
    spectrum_r = jnp.dot(lines, cos_full, precision=lax.Precision.HIGHEST)
    spectrum_i = -jnp.dot(lines, sin_full, precision=lax.Precision.HIGHEST)
    centred = jnp.arange(row_count, dtype=jnp.int32).astype(jnp.float32) - 0.5 * row_count
    angles = 2.0 * math.pi / length * (coef_a * centred)[:, None] * frequency[None, :]
    cosine_turn = jnp.cos(angles)[:, None, :]
    sine_turn = jnp.sin(angles)[:, None, :]
    turned_r = (spectrum_r[None] * cosine_turn - spectrum_i[None] * sine_turn).astype(jnp.bfloat16).reshape(row_count * depth_count, length)
    turned_i = (spectrum_r[None] * sine_turn + spectrum_i[None] * cosine_turn).astype(jnp.bfloat16).reshape(row_count * depth_count, length)
    spread = jnp.dot(turned_r, cos_half, preferred_element_type=jnp.float32) - jnp.dot(turned_i, sin_half, preferred_element_type=jnp.float32)
    return (spread / (length * math.sqrt(length))).reshape(row_count, depth_count, length).astype(jnp.bfloat16)

def patch_gradient(patch, measured, probe_real, probe_imag, dft_cos, dft_sin):

    def product_of(left, right):
        return jnp.dot(left, right, precision=lax.Precision.HIGHEST)
    wave_r = probe_real * jnp.cos(patch) - probe_imag * jnp.sin(patch)
    wave_i = probe_real * jnp.sin(patch) + probe_imag * jnp.cos(patch)
    half_r = product_of(wave_r, dft_cos) + product_of(wave_i, dft_sin)
    half_i = product_of(wave_i, dft_cos) - product_of(wave_r, dft_sin)
    far_r = product_of(dft_cos, half_r) + product_of(dft_sin, half_i)
    far_i = product_of(dft_cos, half_i) - product_of(dft_sin, half_r)
    misfit = far_r * far_r + far_i * far_i - measured
    weighted_r = misfit * far_r
    weighted_i = misfit * far_i
    back_r = product_of(weighted_r, dft_cos) - product_of(weighted_i, dft_sin)
    back_i = product_of(weighted_i, dft_cos) + product_of(weighted_r, dft_sin)
    exit_r = product_of(dft_cos, back_r) - product_of(dft_sin, back_i)
    exit_i = product_of(dft_cos, back_i) + product_of(dft_sin, back_r)
    return 2.0 * (exit_i * wave_r - exit_r * wave_i)

def reference(volume, phase, dual, probe_real, probe_imag, intensity, offsets, angle_index):
    length = volume.shape[2]
    width = probe_real.shape[1]
    cos_full, sin_full = dft_tables(length)
    cos_half = cos_full.astype(jnp.bfloat16)
    sin_half = sin_full.astype(jnp.bfloat16)
    frequency = signed_freq(length)
    centred = jnp.arange(length, dtype=jnp.int32).astype(jnp.float32) - 0.5 * length
    probe_cos, probe_sin = dft_tables(width)
    dft_cos = probe_cos / math.sqrt(width)
    dft_sin = probe_sin / math.sqrt(width)

    def project_all(volume_now):
        rounded = volume_now.astype(jnp.bfloat16)

        def one_angle(angle_number):
            coef_a, coef_b = shear_coefficients(angle_number)
            first = shear_last(rounded, coef_a * centred, cos_half, sin_half, frequency).astype(jnp.bfloat16)
            second = shear_first(first, coef_b * centred, cos_half, sin_half, frequency).astype(jnp.bfloat16)
            return project_lines(second, coef_a, cos_half, sin_half, cos_full, sin_full, frequency)
        return lax.map(one_angle, angle_index)
    proj_old = project_all(volume)

    def angle_gradient(inputs):
        image, corners, measured_all = inputs

        def add_position(position, gradient_image):
            corner = corners[position]
            patch = lax.dynamic_slice_in_dim(image, corner, width, 1)
            term = patch_gradient(patch, measured_all[position], probe_real, probe_imag, dft_cos, dft_sin)
            current = lax.dynamic_slice_in_dim(gradient_image, corner, width, 1)
            return lax.dynamic_update_slice_in_dim(gradient_image, current + term, corner, 1)
        return lax.fori_loop(0, corners.shape[0], add_position, jnp.zeros_like(image))
    gradients = lax.map(angle_gradient, (phase, offsets, intensity))
    phase_new = phase - eta_step * (gradients + dual + rho_weight * (phase - proj_old))
    resid = rho_weight * (proj_old - phase_new) - dual

    def add_angle(total, inputs):
        angle_number, lines = inputs
        coef_a, coef_b = shear_coefficients(angle_number)
        spread = back_lines(lines, length, coef_a, cos_half, sin_half, cos_full, sin_full, frequency)
        second = shear_first(spread, -(coef_b * centred), cos_half, sin_half, frequency).astype(jnp.bfloat16)
        third = shear_last(second, -(coef_a * centred), cos_half, sin_half, frequency)
        return (total + third, None)
    back, unused = lax.scan(add_angle, jnp.zeros(volume.shape, jnp.float32), (angle_index, resid))
    padded = jnp.pad(volume, ((0, 0), (1, 1), (0, 0)))
    smooth = 2.0 * volume - padded[:, :-2, :] - padded[:, 2:, :]
    volume_new = volume - tau_step * (back + smooth_weight * smooth)
    proj_new = project_all(volume_new)
    dual_new = dual + rho_weight * (phase_new - proj_new)
    return (phase_new, volume_new, dual_new)
```

```python
import math

import jax
import jax.numpy as jnp
import numpy as np
from jax import lax
from jax.experimental import pallas as pl
from jax.experimental.pallas import tpu as pltpu
from jax.sharding import PartitionSpec as P

angle_center = 90.0
rho_weight = 1.0
eta_step = 0.01
tau_step = 1.0
smooth_weight = 0.25

N = 256
HALF = 128
PEERS = 8
TILES = 16
ROWS = 16
SHOTS = 4
F32 = jnp.float32
BF16 = jnp.bfloat16
MESH = pl.DeviceIdType.MESH


def tables_of(length):
    index = np.arange(length)
    phases = (index[:, None] * index[None, :] % length).astype(np.float32)
    phases = phases * np.float32(2.0 * math.pi / length)
    return np.cos(phases), np.sin(phases)


def packed_tables():
    cos, sin = tables_of(N)
    signs = np.where(np.arange(N) % 2 == 0, 1.0, -1.0)
    forward = np.concatenate([cos[:, :HALF], -sin[:, :HALF]], axis=1)
    forward[:, HALF] = signs
    inverse = np.concatenate([2.0 * cos[:HALF], -2.0 * sin[:HALF]], axis=0)
    inverse[0] = 1.0
    inverse[HALF] = signs
    inverse = inverse / N
    cos, sin = tables_of(HALF)
    cos, sin = cos / math.sqrt(HALF), sin / math.sqrt(HALF)
    near = np.block([[cos, -sin], [sin, cos]])
    away = np.block([[cos, sin], [-sin, cos]])
    stack = np.stack([forward, inverse, forward.T, inverse.T, near, away])
    return stack.astype(np.float32)


def sincos_turns(turns):
    a = (turns - jnp.floor(turns + 0.5)) * math.pi
    z = a * a
    sin = 1.0
    for k in (12, 10, 8, 6, 4, 2):
        sin = 1.0 - z * sin * (1.0 / (k * (k + 1)))
    sin = a * sin
    cos = 1.0
    for k in (13, 11, 9, 7, 5, 3, 1):
        cos = 1.0 - z * cos * (1.0 / (k * (k + 1)))
    return 2.0 * sin * cos, 1.0 - 2.0 * sin * sin


def dot(a, b):
    return jnp.dot(a, b, preferred_element_type=F32)


def two_parts(x):
    high = x.astype(BF16)
    low = (x - high.astype(F32)).astype(BF16)
    return jnp.concatenate([high, low], axis=0)


def dot_parts(x, table):
    both = dot(two_parts(x), table)
    return both[: x.shape[0]] + both[x.shape[0] :]


def step_kernel(
    offsets_ref, angle_ref, vol_ref, phase_ref, dual_ref, pr_ref, pi_ref, inten_ref, tab_ref,
    phase_out, vol_out, dual_out,
    coef_send, coef_all, v_send, v_all, b_send, b_all, b_own, halo, phase_all, g_send, g_all, l_send, l_all,
    old_send, old_all, new_send, new_all, k_send, k_all, s_send, s_recv,
    tab_a, tab_b, xs, xb, s_sum, spec, wave,
    phase_ss, phase_rs, g_ss, g_rs, coef_ss, coef_rs, v_ss, v_rs, b_ss, b_rs, l_ss, l_rs,
    old_ss, old_rs, new_ss, new_rs, k_ss, k_rs, one_ss, one_rs,
):
    me = lax.axis_index("ang")
    tile = lax.axis_index("tile")
    core = me % 2
    mine = me // 2
    x_me, hi_me = mine // 2, mine % 2
    low = tile % 4
    far_tile = (tile // 4) * 4 + (low + 2) % 4
    turn_out = (low + 2) // 4
    turn_in = ((low + 2) % 4 + 2) // 4
    my_slot = 2 * x_me + (hi_me + turn_in) % 2
    twin = (me - core + (1 - core), tile)

    def peer(p):
        return (2 * p + core, far_tile)

    def slot_of(p):
        return 2 * (p // 2) + (p % 2 + turn_out) % 2

    def beside(o):
        return (me, (tile + o) % TILES)

    barrier = pltpu.get_barrier_semaphore()
    for o in range(1, TILES):
        pl.semaphore_signal(barrier, inc=1, device_id=beside(o), device_id_type=MESH)
    for p in range(PEERS):
        pl.semaphore_signal(barrier, inc=1, device_id=peer(p), device_id_type=MESH)
    pl.semaphore_signal(barrier, inc=1, device_id=twin, device_id_type=MESH)

    fwd_x, inv_x, fwd_y, inv_y, near, away = (tab_ref[i] for i in range(6))

    number = jnp.full((8, 128), angle_ref[0], jnp.int32).astype(F32) - angle_center
    sin_b, unused = sincos_turns(number * (1.0 / 720.0))
    sin_h, cos_h = sincos_turns(number * (1.0 / 1440.0))
    rows8 = lax.broadcasted_iota(jnp.int32, (8, 128), 0)
    coef_send[...] = jnp.where(rows8 < 4, -(sin_h / cos_h), sin_b)
    for q in range(PEERS):
        v_send[q] = vol_ref[:, q, :].astype(BF16)

    pl.semaphore_wait(barrier, TILES + PEERS)

    def copy(src, dst, send, recv, device):
        return pltpu.make_async_remote_copy(
            src_ref=src, dst_ref=dst, send_sem=send, recv_sem=recv, device_id=device, device_id_type=MESH
        )

    def phase_copy(o, slot):
        return copy(phase_ref, phase_all.at[slot], phase_ss.at[o], phase_rs.at[o], beside(o))

    def coef_copy(p, slot, idx):
        return copy(coef_send, coef_all.at[slot], coef_ss.at[p], coef_rs.at[idx], peer(p))

    def v_copy(p, slot, idx):
        return copy(v_send.at[slot_of(p)], v_all.at[slot, core], v_ss.at[p], v_rs.at[idx], peer(p))

    def b_copy(p, slot, idx):
        return copy(b_send.at[slot_of(p)], b_all.at[slot, core], b_ss.at[p], b_rs.at[idx], peer(p))

    def g_copy(o, slot):
        return copy(g_send.at[(tile + o) % TILES], g_all.at[slot], g_ss.at[o], g_rs.at[o], beside(o))

    def l_copy(p, slot, idx):
        return copy(l_send.at[slot_of(p)], l_all.at[slot], l_ss.at[p], l_rs.at[idx], peer(p))

    def old_copy(p, slot, idx):
        return copy(old_send.at[p], old_all.at[slot], old_ss.at[p], old_rs.at[idx], peer(p))

    def new_copy(p, slot, idx):
        return copy(new_send.at[p], new_all.at[slot], new_ss.at[p], new_rs.at[idx], peer(p))

    def k_copy(p, slot, idx):
        return copy(k_send.at[p], k_all.at[slot], k_ss.at[p], k_rs.at[idx], peer(p))

    v_twin = copy(v_all.at[:, core], v_all.at[:, core], one_ss.at[0], one_rs.at[0], twin)
    b_twin = copy(b_all.at[:, core], b_all.at[:, core], one_ss.at[1], one_rs.at[1], twin)
    s_twin = copy(s_send, s_recv, one_ss.at[2], one_rs.at[2], twin)
    halo_up = copy(v_send.at[PEERS - 1], halo.at[0], one_ss.at[3], one_rs.at[3], beside(1))
    halo_down = copy(v_send.at[0], halo.at[1], one_ss.at[4], one_rs.at[4], beside(TILES - 1))

    for o in range(1, TILES):
        phase_copy(o, tile).start()
    for p in range(PEERS):
        coef_copy(p, mine, mine).start()
    for p in range(PEERS):
        v_copy(p, mine, mine).start()
    halo_up.start()
    halo_down.start()
    phase_all[tile] = phase_ref[...]

    for p in range(PEERS):
        coef_copy(p, p, p).wait_recv()

    lane = lax.broadcasted_iota(jnp.int32, (N, HALF), 1)
    line = lax.broadcasted_iota(jnp.int32, (N, HALF), 0)
    freq_a = jnp.where(lane == 0, HALF, lane).astype(F32) * (1.0 / N)
    row_a = (line - HALF).astype(F32)
    lane_b = lax.broadcasted_iota(jnp.int32, (HALF, N), 1)
    line_b = lax.broadcasted_iota(jnp.int32, (HALF, N), 0)
    freq_b = jnp.where(line_b == 0, HALF, line_b).astype(F32) * (1.0 / N)
    row_b = (lane_b - HALF).astype(F32)

    def angle_tables(p, carry):
        coef = coef_all[p]
        shift = coef[0:1, :]
        sin, cos = sincos_turns((row_a * shift) * freq_a)
        tab_a[p, 0] = jnp.where(lane == 0, 1.0, cos)
        tab_a[p, 1] = jnp.where(lane == 0, 0.0, sin)
        tab_a[p, 2] = cos
        shift = jnp.concatenate([coef[4:5, :], coef[4:5, :]], axis=1)
        sin, cos = sincos_turns((row_b * shift) * freq_b)
        tab_b[p, 0] = jnp.where(line_b == 0, 1.0, cos)
        tab_b[p, 1] = jnp.where(line_b == 0, 0.0, sin)
        tab_b[p, 2] = cos
        return carry

    lax.fori_loop(0, PEERS, angle_tables, 0)

    for o in range(1, TILES):
        phase_copy(o, (tile + TILES - o) % TILES).wait_recv()

    sin, cos = sincos_turns(phase_all[...].reshape(BAND_ROWS, N) * (1.0 / (2.0 * math.pi)))
    parts = []
    for s in range(SHOTS):
        back = (N - offsets_ref[0, s]) % N
        c, n = pltpu.roll(cos, back, 1)[:, :HALF], pltpu.roll(sin, back, 1)[:, :HALF]
        wave_r = pr_ref[...] * c - pi_ref[...] * n
        wave_i = pr_ref[...] * n + pi_ref[...] * c
        wave[s, 0] = wave_r
        wave[s, 1] = wave_i
        parts.append(jnp.concatenate([wave_r, wave_i], axis=1).astype(BF16))
    half = dot(jnp.concatenate(parts, axis=0), near).astype(BF16)
    beams = [half[s * HALF : (s + 1) * HALF] for s in range(SHOTS)]
    beams = [jnp.concatenate([b[:, :HALF], b[:, HALF:]], axis=0) for b in beams]
    far = dot(away, jnp.concatenate(beams, axis=1))
    far_r, far_i = far[:HALF], far[HALF:]
    measured = jnp.concatenate([inten_ref[s] for s in range(SHOTS)], axis=1)
    misfit = far_r * far_r + far_i * far_i - measured
    weighted = jnp.concatenate([misfit * far_r, misfit * far_i], axis=0).astype(BF16)
    half = dot(near, weighted).astype(BF16)
    beams = [half[:, s * HALF : (s + 1) * HALF] for s in range(SHOTS)]
    beams = [jnp.concatenate([b[:HALF], b[HALF:]], axis=1) for b in beams]
    leave = dot(jnp.concatenate(beams, axis=0), away)
    image = jnp.zeros((BAND_ROWS, N), F32)
    for s in range(SHOTS):
        e = leave[s * HALF : (s + 1) * HALF]
        term = 2.0 * (e[:, HALF:] * wave[s, 0] - e[:, :HALF] * wave[s, 1])
        wide = jnp.concatenate([term, jnp.zeros((BAND_ROWS, N - HALF), F32)], axis=1)
        image = image + pltpu.roll(wide, offsets_ref[0, s], 1)
    g_send[...] = image.reshape(TILES, 8, N).astype(BF16)
    for o in range(1, TILES):
        g_copy(o, tile).start()
    g_all[tile] = g_send[tile]

    for p in range(PEERS):
        v_copy(p, p, p).wait_recv()
    v_twin.start()
    halo_up.wait_recv()
    halo_down.wait_recv()
    lower = jnp.where(tile > 0, halo[0].astype(F32), 0.0)
    upper = jnp.where(tile < TILES - 1, halo[1].astype(F32), 0.0)
    for q in range(PEERS):
        here = vol_ref[:, q, :]
        before = lower if q == 0 else vol_ref[:, q - 1, :]
        after = upper if q == PEERS - 1 else vol_ref[:, q + 1, :]
        value = here - (tau_step * smooth_weight) * (2.0 * here - before - after)
        b_own[q] = value
        b_send[q] = value.astype(BF16)
    for p in range(PEERS):
        b_copy(p, mine, mine).start()
    copy(v_all.at[:, 1 - core], v_all.at[:, 1 - core], one_ss.at[0], one_rs.at[0], twin).wait_recv()
    xs[...] = dot(v_all[...].reshape(N, N), fwd_x)

    def turned(p_part, q_part, table, p, sign):
        cos, sin, end = table[p, 0], table[p, 1], table[p, 2]
        if sign > 0:
            return p_part * cos + q_part * sin, q_part * end - p_part * sin
        return p_part * cos - q_part * sin, q_part * end + p_part * sin

    def sheared_y(u, p, sign):
        y = dot(fwd_y, u)
        turn = turned(y[:HALF], y[HALF:], tab_b, p, sign)
        return dot(inv_y, jnp.concatenate(turn, axis=0).astype(BF16)).astype(BF16)

    def project(p, carry):
        turn = turned(xs[:, :HALF], xs[:, HALF:], tab_a, p, 1)
        u = dot(jnp.concatenate(turn, axis=1).astype(BF16), inv_x).astype(BF16)
        y = dot(sheared_y(u, p, 1), fwd_x)
        turn = turned(y[:, :HALF], y[:, HALF:], tab_a, p, 1)
        spec[pl.ds(p, 1), :] = jnp.sum(jnp.concatenate(turn, axis=1), axis=0, keepdims=True)
        return carry

    lax.fori_loop(0, PEERS, project, 0)
    old = dot_parts(spec[...], inv_x) * (1.0 / math.sqrt(N))
    for p in range(PEERS):
        old_send[p] = old[p : p + 1]
    for p in range(PEERS):
        old_copy(p, my_slot, my_slot).start()

    for o in range(1, TILES):
        g_copy(o, (tile + TILES - o) % TILES).wait_recv()
    grad = jnp.sum(g_all[...].astype(F32), axis=0)
    base = phase_ref[...] - eta_step * (grad + dual_ref[...] + rho_weight * phase_ref[...])
    lines = rho_weight * base + dual_ref[...]
    for q in range(PEERS):
        l_send[q] = lines[q : q + 1]
    for p in range(PEERS):
        l_copy(p, mine, mine).start()

    for p in range(PEERS):
        b_copy(p, p, p).wait_recv()
    b_twin.start()
    copy(b_all.at[:, 1 - core], b_all.at[:, 1 - core], one_ss.at[1], one_rs.at[1], twin).wait_recv()
    xb[...] = dot(b_all[...].reshape(N, N), fwd_x)

    for p in range(PEERS):
        l_copy(p, p, p).wait_recv()
    asked = jnp.concatenate([l_all[p] for p in range(PEERS)], axis=0)
    resid = (rho_weight * (1.0 - eta_step * rho_weight)) * old - asked
    spec[...] = dot_parts(resid, fwd_x) * (1.0 / math.sqrt(N))
    s_sum[...] = jnp.zeros((N, N), F32)

    def backproject(p, carry):
        g = spec[pl.ds(p, 1), :]
        turn = turned(g[:, :HALF], g[:, HALF:], tab_a, p, -1)
        u = dot(jnp.concatenate(turn, axis=1).astype(BF16), inv_x).astype(BF16)
        y = dot(sheared_y(u, p, -1), fwd_x)
        turn = turned(y[:, :HALF], y[:, HALF:], tab_a, p, -1)
        s_sum[...] += jnp.concatenate(turn, axis=1)
        return carry

    lax.fori_loop(0, PEERS, backproject, 0)
    s_send[...] = s_sum[...].astype(BF16)
    s_twin.start()
    s_twin.wait_recv()
    total = s_sum[...] + s_recv[...].astype(F32)
    xs[...] = xb[...] - tau_step * total
    blocks = total.astype(BF16).reshape(PEERS, 2, ROWS, N)
    blocks = jnp.where(core == 0, blocks[:, 0], blocks[:, 1]).reshape(HALF, N)
    k_send[...] = dot(blocks, inv_x).astype(BF16).reshape(PEERS, ROWS, N)
    for p in range(PEERS):
        k_copy(p, my_slot, my_slot).start()

    lax.fori_loop(0, PEERS, project, 0)
    new = dot_parts(spec[...], inv_x) * (1.0 / math.sqrt(N))
    for p in range(PEERS):
        new_send[p] = new[p : p + 1]
    for p in range(PEERS):
        new_copy(p, my_slot, my_slot).start()

    for p in range(PEERS):
        k_copy(p, slot_of(p), slot_of(p)).wait_recv()
    for q in range(PEERS):
        vol_out[:, q, :] = b_own[q] - tau_step * k_all[q].astype(F32)
    for p in range(PEERS):
        old_copy(p, slot_of(p), slot_of(p)).wait_recv()
    phase_new = base + (eta_step * rho_weight) * jnp.concatenate([old_all[q] for q in range(PEERS)], axis=0)
    phase_out[...] = phase_new
    for p in range(PEERS):
        new_copy(p, slot_of(p), slot_of(p)).wait_recv()
    after = jnp.concatenate([new_all[q] for q in range(PEERS)], axis=0)
    dual_out[...] = dual_ref[...] + rho_weight * (phase_new - after)

    for o in range(1, TILES):
        phase_copy(o, tile).wait_send()
        g_copy(o, tile).wait_send()
    for p in range(PEERS):
        coef_copy(p, mine, mine).wait_send()
        v_copy(p, mine, mine).wait_send()
        b_copy(p, mine, mine).wait_send()
        l_copy(p, mine, mine).wait_send()
        old_copy(p, my_slot, my_slot).wait_send()
        new_copy(p, my_slot, my_slot).wait_send()
        k_copy(p, my_slot, my_slot).wait_send()
    for one in (v_twin, b_twin, s_twin, halo_up, halo_down):
        one.wait_send()


BAND_ROWS = 128


def shards(volume, phase, dual, probe_real, probe_imag, intensity, offsets, angle_index):
    tables = jnp.asarray(packed_tables()).astype(BF16)
    in_vmem = pl.BlockSpec(memory_space=pltpu.VMEM)
    in_smem = pl.BlockSpec(memory_space=pltpu.SMEM)
    dma = pltpu.SemaphoreType.DMA
    vmem = pltpu.VMEM
    blocks = (PEERS, ROWS, N)
    lines = (PEERS, 1, N)
    phase_new, volume_new, dual_new = pl.pallas_call(
        step_kernel,
        out_shape=(
            jax.ShapeDtypeStruct(phase.shape[1:], F32),
            jax.ShapeDtypeStruct(volume.shape, F32),
            jax.ShapeDtypeStruct(dual.shape[1:], F32),
        ),
        in_specs=[in_smem] * 2 + [in_vmem] * 7,
        out_specs=(in_vmem,) * 3,
        scratch_shapes=[
            vmem((8, 128), F32),
            vmem((PEERS, 8, 128), F32),
            vmem(blocks, BF16),
            vmem((PEERS, 2, ROWS, N), BF16),
            vmem(blocks, BF16),
            vmem((PEERS, 2, ROWS, N), BF16),
            vmem(blocks, F32),
            vmem((2, ROWS, N), BF16),
            vmem((TILES, 8, N), F32),
            vmem((TILES, 8, N), BF16),
            vmem((TILES, 8, N), BF16),
            vmem(lines, F32),
            vmem(lines, F32),
            vmem(lines, F32),
            vmem(lines, F32),
            vmem(lines, F32),
            vmem(lines, F32),
            vmem(blocks, BF16),
            vmem(blocks, BF16),
            vmem((N, N), BF16),
            vmem((N, N), BF16),
            vmem((PEERS, 3, N, HALF), F32),
            vmem((PEERS, 3, HALF, N), F32),
            vmem((N, N), F32),
            vmem((N, N), F32),
            vmem((N, N), F32),
            vmem((PEERS, N), F32),
            vmem((SHOTS, 2, HALF, HALF), F32),
            dma((TILES,)),
            dma((TILES,)),
            dma((TILES,)),
            dma((TILES,)),
        ]
        + [dma((PEERS,))] * 14
        + [dma((5,))] * 2,
        compiler_params=pltpu.CompilerParams(collective_id=0, has_side_effects=True),
    )(offsets, angle_index, volume, phase[0], dual[0], probe_real, probe_imag, intensity[0], tables)
    return (phase_new[None], volume_new, dual_new[None])


def solution(mesh):
    placed = (
        P("ang", "tile", None),
        P("ang", "tile", None),
        P("ang", "tile", None),
        P(),
        P(),
        P("ang", "tile", None, None),
        P("ang", "tile"),
        P("ang"),
    )
    return jax.shard_map(
        shards,
        mesh=mesh,
        in_specs=placed,
        out_specs=(P("ang", "tile", None), P("ang", "tile", None), P("ang", "tile", None)),
        check_vma=False,
    )
```

```python
import math

import jax
import jax.numpy as jnp
import numpy as np
from jax import lax
from jax.experimental import pallas as pl
from jax.experimental.pallas import tpu as pltpu
from jax.sharding import PartitionSpec as P

angle_center = 90.0
rho_weight = 1.0
eta_step = 0.01
tau_step = 1.0
smooth_weight = 0.25

N = 256
HALF = 128
PEERS = 8
TILES = 16
ROWS = 16
SHOTS = 4
BAND_ROWS = 128
EARLY = 6
NEAR_LAST = [4 * dy + dz for dy in (2, 1, 3, 0) for dz in range(4) if dy or dz]
F32 = jnp.float32
BF16 = jnp.bfloat16
MESH = pl.DeviceIdType.MESH


def tables_of(length):
    index = np.arange(length)
    phases = (index[:, None] * index[None, :] % length).astype(np.float32)
    phases = phases * np.float32(2.0 * math.pi / length)
    return np.cos(phases), np.sin(phases)


def packed_tables():
    cos, sin = tables_of(N)
    signs = np.where(np.arange(N) % 2 == 0, 1.0, -1.0)
    forward = np.concatenate([cos[:, :HALF], -sin[:, :HALF]], axis=1)
    forward[:, HALF] = signs
    inverse = np.concatenate([2.0 * cos[:HALF], -2.0 * sin[:HALF]], axis=0)
    inverse[0] = 1.0
    inverse[HALF] = signs
    inverse = inverse / N
    cos, sin = tables_of(HALF)
    cos, sin = cos / math.sqrt(HALF), sin / math.sqrt(HALF)
    near = np.block([[cos, -sin], [sin, cos]])
    away = np.block([[cos, sin], [-sin, cos]])
    stack = np.stack([forward, inverse, forward.T, inverse.T, near, away])
    return stack.astype(np.float32)


def sincos_turns(turns):
    a = (turns - jnp.floor(turns + 0.5)) * math.pi
    z = a * a
    sin = 1.0
    for k in (12, 10, 8, 6, 4, 2):
        sin = 1.0 - z * sin * (1.0 / (k * (k + 1)))
    sin = a * sin
    cos = 1.0
    for k in (13, 11, 9, 7, 5, 3, 1):
        cos = 1.0 - z * cos * (1.0 / (k * (k + 1)))
    return 2.0 * sin * cos, 1.0 - 2.0 * sin * sin


def dot(a, b):
    return jnp.dot(a, b, preferred_element_type=F32)


def two_parts(x):
    high = x.astype(BF16)
    low = (x - high.astype(F32)).astype(BF16)
    return jnp.concatenate([high, low], axis=0)


def dot_parts(x, table):
    both = dot(two_parts(x), table)
    return both[: x.shape[0]] + both[x.shape[0] :]


def step_kernel(
    offsets_in, angle_in, vol_in, phase_in, dual_in, pr_in, pi_in, inten_in, tab_in,
    phase_out, vol_out, dual_out,
    offsets_ref, angle_ref, vol_ref, phase_ref, dual_ref, pr_ref, pi_ref, inten_ref, tab_ref, phase_send,
    coef_send, coef_all, v_send, v_all, b_send, b_all, b_own, halo, phase_all, g_send, g_all, l_send, l_all,
    old_send, old_all, new_send, new_all, k_send, k_all, s_send, s_recv,
    tab_a, tab_b, xs, xb, s_sum, wave,
    phase_ss, phase_rs, g_ss, g_rs, coef_ss, coef_rs, v_ss, v_rs, b_ss, b_rs, l_ss, l_rs,
    old_ss, old_rs, new_ss, new_rs, k_ss, k_rs, one_ss, one_rs, in_sem,
):
    me = lax.axis_index("ang")
    tile = lax.axis_index("tile")
    core = me % 2
    mine = me // 2
    x_me, hi_me = mine // 2, mine % 2
    low = tile % 4
    far_tile = (tile // 4) * 4 + (low + 2) % 4
    turn_out = (low + 2) // 4
    turn_in = ((low + 2) % 4 + 2) // 4
    my_slot = 2 * x_me + (hi_me + turn_in) % 2
    twin = (me - core + (1 - core), tile)

    def peer(p):
        return (2 * p + core, far_tile)

    def slot_of(p):
        return 2 * (p // 2) + (p % 2 + turn_out) % 2

    def beside(o):
        return (me, ((tile // 4 + o // 4) % 4) * 4 + (low + o) % 4)

    def sender(o):
        return ((tile // 4 + 4 - o // 4) % 4) * 4 + (low + 4 - o % 4) % 4

    order = [2 * ((x_me + dx) % 4) + zh for dx in (2, 1, 3, 0) for zh in (0, 1)]

    barrier = pltpu.get_barrier_semaphore()
    for o in NEAR_LAST:
        pl.semaphore_signal(barrier, inc=1, device_id=beside(o), device_id_type=MESH)
    for p in range(PEERS):
        pl.semaphore_signal(barrier, inc=1, device_id=peer(p), device_id_type=MESH)
    pl.semaphore_signal(barrier, inc=1, device_id=twin, device_id_type=MESH)

    loads = [
        pltpu.make_async_copy(src, dst, in_sem.at[i])
        for i, (src, dst) in enumerate(
            [
                (angle_in, angle_ref), (phase_in, phase_ref), (vol_in, vol_ref), (offsets_in, offsets_ref),
                (pr_in, pr_ref), (pi_in, pi_ref), (inten_in, inten_ref), (tab_in, tab_ref), (dual_in, dual_ref),
            ]
        )
    ]
    for load in loads:
        load.start()

    loads[0].wait()
    number = jnp.full((8, 128), angle_ref[0], jnp.int32).astype(F32) - angle_center
    sin_b, unused = sincos_turns(number * (1.0 / 720.0))
    sin_h, cos_h = sincos_turns(number * (1.0 / 1440.0))
    rows8 = lax.broadcasted_iota(jnp.int32, (8, 128), 0)
    coef_send[...] = jnp.where(rows8 < 4, -(sin_h / cos_h), sin_b)
    loads[1].wait()
    turns = phase_ref[...] * (1.0 / (2.0 * math.pi))
    phase_send[...] = (turns - jnp.floor(turns + 0.5)).astype(BF16)
    loads[2].wait()
    for q in range(PEERS):
        v_send[q] = vol_ref[:, q, :].astype(BF16)

    pl.semaphore_wait(barrier, TILES + PEERS)

    def copy(src, dst, send, recv, device):
        return pltpu.make_async_remote_copy(
            src_ref=src, dst_ref=dst, send_sem=send, recv_sem=recv, device_id=device, device_id_type=MESH
        )

    def phase_copy(o, slot):
        return copy(phase_send, phase_all.at[slot], phase_ss.at[o], phase_rs.at[o], beside(o))

    def coef_copy(p, slot, idx):
        return copy(coef_send, coef_all.at[slot], coef_ss.at[p], coef_rs.at[idx], peer(p))

    def v_copy(p, slot, idx):
        return copy(v_send.at[slot_of(p)], v_all.at[slot, core], v_ss.at[p], v_rs.at[idx], peer(p))

    def b_copy(p, slot, idx):
        return copy(b_send.at[slot_of(p)], b_all.at[slot, core], b_ss.at[p], b_rs.at[idx], peer(p))

    def g_copy(o, slot):
        return copy(g_send.at[beside(o)[1]], g_all.at[slot], g_ss.at[o], g_rs.at[o], beside(o))

    def l_copy(p, slot, idx):
        return copy(l_send.at[slot_of(p)], l_all.at[slot], l_ss.at[p], l_rs.at[idx], peer(p))

    def old_copy(j, p, slot, idx):
        return copy(old_send.at[j], old_all.at[slot], old_ss.at[j], old_rs.at[idx], peer(p))

    def new_copy(j, p, slot, idx):
        return copy(new_send.at[j], new_all.at[slot], new_ss.at[j], new_rs.at[idx], peer(p))

    def k_copy(p, slot, idx):
        return copy(k_send.at[p], k_all.at[slot], k_ss.at[p], k_rs.at[idx], peer(p))

    v_twin = copy(v_all.at[:, core], v_all.at[:, core], one_ss.at[0], one_rs.at[0], twin)
    b_twin = copy(b_all.at[:, core], b_all.at[:, core], one_ss.at[1], one_rs.at[1], twin)
    s_twin = copy(s_send, s_recv, one_ss.at[2], one_rs.at[2], twin)
    halo_up = copy(v_send.at[PEERS - 1], halo.at[0], one_ss.at[3], one_rs.at[3], (me, (tile + 1) % TILES))
    halo_down = copy(v_send.at[0], halo.at[1], one_ss.at[4], one_rs.at[4], (me, (tile + TILES - 1) % TILES))

    for p in range(PEERS):
        coef_copy(p, mine, mine).start()
    for o in NEAR_LAST:
        phase_copy(o, tile).start()
    for p in range(PEERS):
        v_copy(p, mine, mine).start()
    halo_up.start()
    halo_down.start()
    phase_all[tile] = phase_send[...]
    for load in loads[3:]:
        load.wait()
    fwd_x, inv_x, fwd_y, inv_y, near, away = (tab_ref[i] for i in range(6))

    for p in range(PEERS):
        coef_copy(p, p, p).wait_recv()

    lane = lax.broadcasted_iota(jnp.int32, (N, HALF), 1)
    line = lax.broadcasted_iota(jnp.int32, (N, HALF), 0)
    freq_a = jnp.where(lane == 0, HALF, lane).astype(F32) * (1.0 / N)
    row_a = (line - HALF).astype(F32)
    lane_b = lax.broadcasted_iota(jnp.int32, (HALF, N), 1)
    line_b = lax.broadcasted_iota(jnp.int32, (HALF, N), 0)
    freq_b = jnp.where(line_b == 0, HALF, line_b).astype(F32) * (1.0 / N)
    row_b = (lane_b - HALF).astype(F32)

    def angle_tables(p, carry):
        coef = coef_all[p]
        shift = coef[0:1, :]
        sin, cos = sincos_turns((row_a * shift) * freq_a)
        tab_a[p, 0] = jnp.where(lane == 0, 1.0, cos)
        tab_a[p, 1] = jnp.where(lane == 0, 0.0, sin)
        tab_a[p, 2] = cos
        shift = jnp.concatenate([coef[4:5, :], coef[4:5, :]], axis=1)
        sin, cos = sincos_turns((row_b * shift) * freq_b)
        tab_b[p, 0] = jnp.where(line_b == 0, 1.0, cos)
        tab_b[p, 1] = jnp.where(line_b == 0, 0.0, sin)
        tab_b[p, 2] = cos
        return carry

    lax.fori_loop(0, PEERS, angle_tables, 0)

    for o in range(1, TILES):
        phase_copy(o, sender(o)).wait_recv()

    sin, cos = sincos_turns(phase_all[...].astype(F32).reshape(BAND_ROWS, N))
    parts = []
    for s in range(SHOTS):
        back = (N - offsets_ref[0, s]) % N
        c, n = pltpu.roll(cos, back, 1)[:, :HALF], pltpu.roll(sin, back, 1)[:, :HALF]
        wave_r = pr_ref[...] * c - pi_ref[...] * n
        wave_i = pr_ref[...] * n + pi_ref[...] * c
        wave[s, 0] = wave_r
        wave[s, 1] = wave_i
        parts.append(jnp.concatenate([wave_r, wave_i], axis=1).astype(BF16))
    half = dot(jnp.concatenate(parts, axis=0), near).astype(BF16)
    beams = [half[s * HALF : (s + 1) * HALF] for s in range(SHOTS)]
    beams = [jnp.concatenate([b[:, :HALF], b[:, HALF:]], axis=0) for b in beams]
    far = dot(away, jnp.concatenate(beams, axis=1))
    far_r, far_i = far[:HALF], far[HALF:]
    measured = jnp.concatenate([inten_ref[s] for s in range(SHOTS)], axis=1)
    misfit = far_r * far_r + far_i * far_i - measured
    weighted = jnp.concatenate([misfit * far_r, misfit * far_i], axis=0).astype(BF16)
    half = dot(near, weighted).astype(BF16)
    beams = [half[:, s * HALF : (s + 1) * HALF] for s in range(SHOTS)]
    beams = [jnp.concatenate([b[:HALF], b[HALF:]], axis=1) for b in beams]
    leave = dot(jnp.concatenate(beams, axis=0), away)
    image = jnp.zeros((BAND_ROWS, N), F32)
    for s in range(SHOTS):
        e = leave[s * HALF : (s + 1) * HALF]
        term = 2.0 * (e[:, HALF:] * wave[s, 0] - e[:, :HALF] * wave[s, 1])
        wide = jnp.concatenate([term, jnp.zeros((BAND_ROWS, N - HALF), F32)], axis=1)
        image = image + pltpu.roll(wide, offsets_ref[0, s], 1)
    g_send[...] = image.reshape(TILES, 8, N).astype(BF16)
    for o in NEAR_LAST:
        g_copy(o, tile).start()
    g_all[tile] = g_send[tile]

    for p in range(PEERS):
        v_copy(p, p, p).wait_recv()
    v_twin.start()
    halo_up.wait_recv()
    halo_down.wait_recv()
    lower = jnp.where(tile > 0, halo[0].astype(F32), 0.0)
    upper = jnp.where(tile < TILES - 1, halo[1].astype(F32), 0.0)
    for q in range(PEERS):
        here = vol_ref[:, q, :]
        before = lower if q == 0 else vol_ref[:, q - 1, :]
        after = upper if q == PEERS - 1 else vol_ref[:, q + 1, :]
        value = here - (tau_step * smooth_weight) * (2.0 * here - before - after)
        b_own[q] = value
        b_send[q] = value.astype(BF16)
    for p in range(PEERS):
        b_copy(p, mine, mine).start()
    copy(v_all.at[:, 1 - core], v_all.at[:, 1 - core], one_ss.at[0], one_rs.at[0], twin).wait_recv()
    xs[...] = dot(v_all[...].reshape(N, N), fwd_x)

    def turned(p_part, q_part, table, p, sign):
        cos, sin, end = table[p, 0], table[p, 1], table[p, 2]
        if sign > 0:
            return p_part * cos + q_part * sin, q_part * end - p_part * sin
        return p_part * cos - q_part * sin, q_part * end + p_part * sin

    def sheared_y(u, p, sign):
        y = dot(fwd_y, u)
        turn = turned(y[:HALF], y[HALF:], tab_b, p, sign)
        return dot(inv_y, jnp.concatenate(turn, axis=0).astype(BF16)).astype(BF16)

    def project(p):
        turn = turned(xs[:, :HALF], xs[:, HALF:], tab_a, p, 1)
        u = dot(jnp.concatenate(turn, axis=1).astype(BF16), inv_x).astype(BF16)
        y = dot(sheared_y(u, p, 1), fwd_x)
        turn = turned(y[:, :HALF], y[:, HALF:], tab_a, p, 1)
        return jnp.sum(jnp.concatenate(turn, axis=1), axis=0, keepdims=True)

    def lines_of(spectra):
        return dot_parts(jnp.concatenate(spectra, axis=0), inv_x) * (1.0 / math.sqrt(N))

    spectra = [project(p) for p in order[:EARLY]]

    for o in range(1, TILES):
        g_copy(o, sender(o)).wait_recv()
    grad = jnp.sum(g_all[...].astype(F32), axis=0)
    base = phase_ref[...] - eta_step * (grad + dual_ref[...] + rho_weight * phase_ref[...])
    lines = rho_weight * base + dual_ref[...]
    for q in range(PEERS):
        l_send[q] = lines[q : q + 1]
    for p in range(PEERS):
        l_copy(p, mine, mine).start()

    for p in range(PEERS):
        b_copy(p, p, p).wait_recv()
    b_twin.start()
    spectra += [project(p) for p in order[EARLY:]]
    old = lines_of(spectra)
    for j, p in enumerate(order):
        old_send[j] = old[j : j + 1]
    for j, p in enumerate(order):
        old_copy(j, p, my_slot, my_slot).start()
    copy(b_all.at[:, 1 - core], b_all.at[:, 1 - core], one_ss.at[1], one_rs.at[1], twin).wait_recv()
    xb[...] = dot(b_all[...].reshape(N, N), fwd_x)

    for p in range(PEERS):
        l_copy(p, p, p).wait_recv()
    asked = jnp.concatenate([l_all[p] for p in order], axis=0)
    resid = (rho_weight * (1.0 - eta_step * rho_weight)) * old - asked
    asked = dot_parts(resid, fwd_x) * (1.0 / math.sqrt(N))
    s_sum[...] = jnp.zeros((N, N), F32)

    def backproject(j, p):
        g = asked[j : j + 1]
        turn = turned(g[:, :HALF], g[:, HALF:], tab_a, p, -1)
        u = dot(jnp.concatenate(turn, axis=1).astype(BF16), inv_x).astype(BF16)
        y = dot(sheared_y(u, p, -1), fwd_x)
        turn = turned(y[:, :HALF], y[:, HALF:], tab_a, p, -1)
        s_sum[...] += jnp.concatenate(turn, axis=1)

    for j, p in enumerate(order):
        backproject(j, p)
    s_send[...] = s_sum[...].astype(BF16)
    s_twin.start()
    s_twin.wait_recv()
    total = s_sum[...] + s_recv[...].astype(F32)
    xs[...] = xb[...] - tau_step * total
    blocks = total.astype(BF16).reshape(PEERS, 2, ROWS, N)
    blocks = jnp.where(core == 0, blocks[:, 0], blocks[:, 1]).reshape(HALF, N)
    k_send[...] = dot(blocks, inv_x).astype(BF16).reshape(PEERS, ROWS, N)
    for p in range(PEERS):
        k_copy(p, my_slot, my_slot).start()

    for first, last in ((0, 2), (2, 6), (6, 8)):
        new = lines_of([project(p) for p in order[first:last]])
        for j in range(first, last):
            new_send[j] = new[j - first : j - first + 1]
        for j in range(first, last):
            new_copy(j, order[j], my_slot, my_slot).start()

    for p in range(PEERS):
        k_copy(p, slot_of(p), slot_of(p)).wait_recv()
    for q in range(PEERS):
        vol_out[:, q, :] = b_own[q] - tau_step * k_all[q].astype(F32)
    for p in range(PEERS):
        old_copy(p, p, slot_of(p), slot_of(p)).wait_recv()
    phase_new = base + (eta_step * rho_weight) * jnp.concatenate([old_all[q] for q in range(PEERS)], axis=0)
    phase_out[...] = phase_new
    for p in range(PEERS):
        new_copy(p, p, slot_of(p), slot_of(p)).wait_recv()
    after = jnp.concatenate([new_all[q] for q in range(PEERS)], axis=0)
    dual_out[...] = dual_ref[...] + rho_weight * (phase_new - after)

    for o in range(1, TILES):
        phase_copy(o, tile).wait_send()
        g_copy(o, tile).wait_send()
    for p in range(PEERS):
        coef_copy(p, mine, mine).wait_send()
        v_copy(p, mine, mine).wait_send()
        b_copy(p, mine, mine).wait_send()
        l_copy(p, mine, mine).wait_send()
        old_copy(p, order[p], my_slot, my_slot).wait_send()
        new_copy(p, order[p], my_slot, my_slot).wait_send()
        k_copy(p, my_slot, my_slot).wait_send()
    for one in (v_twin, b_twin, s_twin, halo_up, halo_down):
        one.wait_send()


def hand_over(phase_in, vol_in, dual_in, phase_out, vol_out, dual_out):
    phase_out[...] = phase_in[...]
    vol_out[...] = vol_in[...]
    dual_out[...] = dual_in[...]


def shards(volume, phase, dual, probe_real, probe_imag, intensity, offsets, angle_index):
    tables = jnp.asarray(packed_tables()).astype(BF16)
    in_vmem = pl.BlockSpec(memory_space=pltpu.VMEM)
    in_place = pl.BlockSpec(memory_space=pl.ANY)
    dma = pltpu.SemaphoreType.DMA
    vmem = pltpu.VMEM
    blocks = (PEERS, ROWS, N)
    lines = (PEERS, 1, N)
    results = (
        jax.ShapeDtypeStruct(phase.shape[1:], F32),
        jax.ShapeDtypeStruct(volume.shape, F32),
        jax.ShapeDtypeStruct(dual.shape[1:], F32),
    )
    made = pl.pallas_call(
        step_kernel,
        out_shape=results,
        in_specs=[in_place] * 9,
        out_specs=(in_vmem,) * 3,
        scratch_shapes=[
            pltpu.SMEM((1, SHOTS), jnp.int32),
            pltpu.SMEM((1,), jnp.int32),
            vmem(volume.shape, F32),
            vmem((8, N), F32),
            vmem((8, N), F32),
            vmem((HALF, HALF), F32),
            vmem((HALF, HALF), F32),
            vmem((SHOTS, HALF, HALF), F32),
            vmem(tables.shape, BF16),
            vmem((8, N), BF16),
            vmem((8, 128), F32),
            vmem((PEERS, 8, 128), F32),
            vmem(blocks, BF16),
            vmem((PEERS, 2, ROWS, N), BF16),
            vmem(blocks, BF16),
            vmem((PEERS, 2, ROWS, N), BF16),
            vmem(blocks, F32),
            vmem((2, ROWS, N), BF16),
            vmem((TILES, 8, N), BF16),
            vmem((TILES, 8, N), BF16),
            vmem((TILES, 8, N), BF16),
            vmem(lines, F32),
            vmem(lines, F32),
            vmem(lines, F32),
            vmem(lines, F32),
            vmem(lines, F32),
            vmem(lines, F32),
            vmem(blocks, BF16),
            vmem(blocks, BF16),
            vmem((N, N), BF16),
            vmem((N, N), BF16),
            vmem((PEERS, 3, N, HALF), F32),
            vmem((PEERS, 3, HALF, N), F32),
            vmem((N, N), F32),
            vmem((N, N), F32),
            vmem((N, N), F32),
            vmem((SHOTS, 2, HALF, HALF), F32),
            dma((TILES,)),
            dma((TILES,)),
            dma((TILES,)),
            dma((TILES,)),
        ]
        + [dma((PEERS,))] * 14
        + [dma((5,))] * 2
        + [dma((9,))],
        compiler_params=pltpu.CompilerParams(collective_id=0, has_side_effects=True),
    )(offsets, angle_index, volume, phase[0], dual[0], probe_real, probe_imag, intensity[0], tables)
    phase_new, volume_new, dual_new = pl.pallas_call(
        hand_over, out_shape=results, in_specs=[in_vmem] * 3, out_specs=(in_vmem,) * 3
    )(*made)
    return (phase_new[None], volume_new, dual_new[None])


def solution(mesh):
    placed = (
        P("ang", "tile", None),
        P("ang", "tile", None),
        P("ang", "tile", None),
        P(),
        P(),
        P("ang", "tile", None, None),
        P("ang", "tile"),
        P("ang"),
    )
    return jax.shard_map(
        shards,
        mesh=mesh,
        in_specs=placed,
        out_specs=(P("ang", "tile", None), P("ang", "tile", None), P("ang", "tile", None)),
        check_vma=False,
    )
```

```python
import math

import jax
import jax.numpy as jnp
import numpy as np
from jax import lax
from jax.experimental import pallas as pl
from jax.experimental.pallas import tpu as pltpu
from jax.sharding import PartitionSpec as P

angle_center = 90.0
rho_weight = 1.0
eta_step = 0.01
tau_step = 1.0
smooth_weight = 0.25

N = 256
HALF = 128
PEERS = 8
TILES = 16
ROWS = 16
SHOTS = 4
BAND_ROWS = 128
STRIP = 32
FWD_X, INV_X, FWD_Y, INV_Y = range(4)
PHASE, GRAD, COEF, VOLUME, SMOOTH, LINES, OLD, NEW, BACK = range(9)
PARTS = 4
NEAR_LAST = [4 * dy + dz for dy in (2, 1, 3, 0) for dz in range(4) if dy or dz]
F32 = jnp.float32
BF16 = jnp.bfloat16
MESH = pl.DeviceIdType.MESH


def tables_of(length):
    index = np.arange(length)
    phases = (index[:, None] * index[None, :] % length).astype(np.float32)
    phases = phases * np.float32(2.0 * math.pi / length)
    return np.cos(phases), np.sin(phases)


def packed_tables():
    cos, sin = tables_of(N)
    signs = np.where(np.arange(N) % 2 == 0, 1.0, -1.0)
    forward = np.concatenate([cos[:, :HALF], -sin[:, :HALF]], axis=1)
    forward[:, HALF] = signs
    inverse = np.concatenate([2.0 * cos[:HALF], -2.0 * sin[:HALF]], axis=0)
    inverse[0] = 1.0
    inverse[HALF] = signs
    inverse = inverse / N
    cos, sin = tables_of(HALF)
    cos, sin = cos / math.sqrt(HALF), sin / math.sqrt(HALF)
    near = np.block([[cos, -sin], [sin, cos]])
    away = np.block([[cos, sin], [-sin, cos]])
    stack = np.stack([forward, inverse, forward.T, inverse.T, near, away])
    return stack.astype(np.float32)


def sincos_turns(turns):
    a = (turns - jnp.floor(turns + 0.5)) * math.pi
    z = a * a
    sin = 1.0
    for k in (12, 10, 8, 6, 4, 2):
        sin = 1.0 - z * sin * (1.0 / (k * (k + 1)))
    sin = a * sin
    cos = 1.0
    for k in (13, 11, 9, 7, 5, 3, 1):
        cos = 1.0 - z * cos * (1.0 / (k * (k + 1)))
    return 2.0 * sin * cos, 1.0 - 2.0 * sin * sin


def dot(a, b):
    return jnp.dot(a, b, preferred_element_type=F32)


def two_parts(x):
    high = x.astype(BF16)
    low = (x - high.astype(F32)).astype(BF16)
    return jnp.concatenate([high, low], axis=0)


def dot_parts(x, table):
    both = dot(two_parts(x), table)
    return both[: x.shape[0]] + both[x.shape[0] :]


def step_kernel(
    offsets_in, angle_in, vol_in, phase_in, dual_in, pr_in, pi_in, inten_in, tab_in,
    phase_out, vol_out, dual_out,
    offsets_ref, angle_ref, vol_ref, phase_ref, dual_ref, pr_ref, pi_ref, inten_ref, tab_ref, phase_send,
    coef_send, coef_all, v_send, v_all, b_send, b_all, b_own, halo, phase_all, g_send, g_all, l_send, l_all,
    old_send, old_all, new_send, new_all, k_send, k_all, s_send, s_recv,
    work_a, work_b, vol_made, phase_made, dual_made, tab_a, tab_b, xs, xb, s_sum, wave,
    sent, came, one_ss, one_rs, part_ss, part_rs, in_sem,
):
    me = lax.axis_index("ang")
    tile = lax.axis_index("tile")
    core = me % 2
    mine = me // 2
    x_me, hi_me = mine // 2, mine % 2
    low = tile % 4
    far_tile = (tile // 4) * 4 + (low + 2) % 4
    turn_out = (low + 2) // 4
    turn_in = ((low + 2) % 4 + 2) // 4
    my_slot = 2 * x_me + (hi_me + turn_in) % 2
    twin = (me - core + (1 - core), tile)

    def peer(p):
        return (2 * p + core, far_tile)

    def slot_of(p):
        return 2 * (p // 2) + (p % 2 + turn_out) % 2

    def beside(o):
        return (me, ((tile // 4 + o // 4) % 4) * 4 + (low + o) % 4)

    order = [2 * ((x_me + dx) % 4) + zh for dx in (2, 1, 3, 0) for zh in (0, 1)]

    barrier = pltpu.get_barrier_semaphore()
    for o in NEAR_LAST:
        pl.semaphore_signal(barrier, inc=1, device_id=beside(o), device_id_type=MESH)
    for p in range(PEERS):
        pl.semaphore_signal(barrier, inc=1, device_id=peer(p), device_id_type=MESH)
    pl.semaphore_signal(barrier, inc=1, device_id=twin, device_id_type=MESH)

    loads = [
        pltpu.make_async_copy(src, dst, in_sem.at[i])
        for i, (src, dst) in enumerate(
            [
                (angle_in, angle_ref), (phase_in, phase_ref), (vol_in, vol_ref), (offsets_in, offsets_ref),
                (pr_in, pr_ref), (pi_in, pi_ref), (inten_in, inten_ref), (tab_in, tab_ref), (dual_in, dual_ref),
            ]
        )
    ]
    for load in loads:
        load.start()

    loads[0].wait()
    number = jnp.full((8, 128), angle_ref[0], jnp.int32).astype(F32) - angle_center
    sin_b, unused = sincos_turns(number * (1.0 / 720.0))
    sin_h, cos_h = sincos_turns(number * (1.0 / 1440.0))
    rows8 = lax.broadcasted_iota(jnp.int32, (8, 128), 0)
    coef_send[...] = jnp.where(rows8 < 4, -(sin_h / cos_h), sin_b)
    loads[1].wait()
    turns = phase_ref[...] * (1.0 / (2.0 * math.pi))
    phase_send[...] = (turns - jnp.floor(turns + 0.5)).astype(BF16)
    loads[2].wait()
    for q in range(PEERS):
        v_send[q] = vol_ref[:, q, :].astype(BF16)

    pl.semaphore_wait(barrier, TILES + PEERS)

    def copy(src, dst, send, recv, device):
        return pltpu.make_async_remote_copy(
            src_ref=src, dst_ref=dst, send_sem=send, recv_sem=recv, device_id=device, device_id_type=MESH
        )

    def phase_copy(o, slot):
        return copy(phase_send, phase_all.at[slot], sent.at[0], came.at[0], beside(o))

    def coef_copy(p, slot):
        return copy(coef_send, coef_all.at[slot], sent.at[2], came.at[2], peer(p))

    def v_copy(p, slot):
        return copy(v_send.at[slot_of(p)], v_all.at[slot, core], sent.at[3], came.at[3], peer(p))

    def b_copy(p, slot):
        return copy(b_send.at[slot_of(p)], b_all.at[slot, core], sent.at[4], came.at[4], peer(p))

    def g_copy(o, slot):
        return copy(g_send.at[beside(o)[1]], g_all.at[slot], sent.at[1], came.at[1], beside(o))

    def l_copy(p, slot):
        return copy(l_send.at[slot_of(p)], l_all.at[slot], sent.at[5], came.at[5], peer(p))

    def old_copy(j, p, slot):
        return copy(old_send.at[j], old_all.at[slot], sent.at[6], came.at[6], peer(p))

    def new_copy(j, p, slot):
        return copy(new_send.at[j], new_all.at[slot], sent.at[7], came.at[7], peer(p))

    def k_copy(p, slot):
        return copy(k_send.at[p], k_all.at[slot], sent.at[8], came.at[8], peer(p))

    others = pl.ds(0, TILES - 1)
    groups = [phase_all.at[others], g_all.at[others], coef_all, v_send, b_send, l_send, old_send, new_send, k_send]

    def arrived(group):
        copy(groups[group], groups[group], sent.at[group], came.at[group], twin).wait_recv()

    v_twin = copy(v_all.at[:, core], v_all.at[:, core], one_ss.at[0], one_rs.at[0], twin)
    b_twin = copy(b_all.at[:, core], b_all.at[:, core], one_ss.at[1], one_rs.at[1], twin)
    parts = [slice(r, r + N // PARTS) for r in range(0, N, N // PARTS)]
    s_twins = [
        copy(s_send.at[rows], s_recv.at[rows], part_ss.at[i], part_rs.at[i], twin) for i, rows in enumerate(parts)
    ]
    halo_up = copy(v_send.at[PEERS - 1], halo.at[0], one_ss.at[2], one_rs.at[2], (me, (tile + 1) % TILES))
    halo_down = copy(v_send.at[0], halo.at[1], one_ss.at[3], one_rs.at[3], (me, (tile + TILES - 1) % TILES))

    for p in range(PEERS):
        coef_copy(p, mine).start()
    for o in NEAR_LAST:
        phase_copy(o, tile).start()
    for p in range(PEERS):
        v_copy(p, mine).start()
    halo_up.start()
    halo_down.start()
    phase_all[tile] = phase_send[...]
    for load in loads[3:]:
        load.wait()
    near, away = tab_ref[4], tab_ref[5]

    arrived(PHASE)

    sin, cos = sincos_turns(phase_all[...].astype(F32).reshape(BAND_ROWS, N))
    waves = []
    for s in range(SHOTS):
        back = (N - offsets_ref[0, s]) % N
        c, n = pltpu.roll(cos, back, 1)[:, :HALF], pltpu.roll(sin, back, 1)[:, :HALF]
        wave_r = pr_ref[...] * c - pi_ref[...] * n
        wave_i = pr_ref[...] * n + pi_ref[...] * c
        wave[s, 0] = wave_r
        wave[s, 1] = wave_i
        waves.append(jnp.concatenate([wave_r, wave_i], axis=1).astype(BF16))
    half = dot(jnp.concatenate(waves, axis=0), near).astype(BF16)
    beams = [half[s * HALF : (s + 1) * HALF] for s in range(SHOTS)]
    beams = [jnp.concatenate([b[:, :HALF], b[:, HALF:]], axis=0) for b in beams]
    far = dot(away, jnp.concatenate(beams, axis=1))
    far_r, far_i = far[:HALF], far[HALF:]
    measured = jnp.concatenate([inten_ref[s] for s in range(SHOTS)], axis=1)
    misfit = far_r * far_r + far_i * far_i - measured
    weighted = jnp.concatenate([misfit * far_r, misfit * far_i], axis=0).astype(BF16)
    half = dot(near, weighted).astype(BF16)
    beams = [half[:, s * HALF : (s + 1) * HALF] for s in range(SHOTS)]
    beams = [jnp.concatenate([b[:HALF], b[HALF:]], axis=1) for b in beams]
    leave = dot(jnp.concatenate(beams, axis=0), away)
    image = jnp.zeros((BAND_ROWS, N), F32)
    for s in range(SHOTS):
        e = leave[s * HALF : (s + 1) * HALF]
        term = 2.0 * (e[:, HALF:] * wave[s, 0] - e[:, :HALF] * wave[s, 1])
        wide = jnp.concatenate([term, jnp.zeros((BAND_ROWS, N - HALF), F32)], axis=1)
        image = image + pltpu.roll(wide, offsets_ref[0, s], 1)
    g_send[...] = image.reshape(TILES, 8, N).astype(BF16)
    for o in NEAR_LAST:
        g_copy(o, tile).start()
    g_all[tile] = g_send[tile]
    halo_up.wait_recv()
    halo_down.wait_recv()
    lower = jnp.where(tile > 0, halo[0].astype(F32), 0.0)
    upper = jnp.where(tile < TILES - 1, halo[1].astype(F32), 0.0)
    for q in range(PEERS):
        here = vol_ref[:, q, :]
        before = lower if q == 0 else vol_ref[:, q - 1, :]
        after = upper if q == PEERS - 1 else vol_ref[:, q + 1, :]
        value = here - (tau_step * smooth_weight) * (2.0 * here - before - after)
        b_own[q] = value
        b_send[q] = value.astype(BF16)
    for p in range(PEERS):
        b_copy(p, mine).start()

    arrived(COEF)

    lane = lax.broadcasted_iota(jnp.int32, (N, HALF), 1)
    line = lax.broadcasted_iota(jnp.int32, (N, HALF), 0)
    freq_a = jnp.where(lane == 0, HALF, lane).astype(F32) * (1.0 / N)
    row_a = (line - HALF).astype(F32)
    lane_b = lax.broadcasted_iota(jnp.int32, (HALF, N), 1)
    line_b = lax.broadcasted_iota(jnp.int32, (HALF, N), 0)
    freq_b = jnp.where(line_b == 0, HALF, line_b).astype(F32) * (1.0 / N)
    row_b = (lane_b - HALF).astype(F32)

    def angle_tables(p, carry):
        coef = coef_all[p]
        shift = coef[0:1, :]
        sin, cos = sincos_turns((row_a * shift) * freq_a)
        tab_a[p, 0] = jnp.where(lane == 0, 1.0, cos)
        tab_a[p, 1] = jnp.where(lane == 0, 0.0, sin)
        tab_a[p, 2] = cos
        shift = jnp.concatenate([coef[4:5, :], coef[4:5, :]], axis=1)
        sin, cos = sincos_turns((row_b * shift) * freq_b)
        tab_b[p, 0] = jnp.where(line_b == 0, 1.0, cos)
        tab_b[p, 1] = jnp.where(line_b == 0, 0.0, sin)
        tab_b[p, 2] = cos
        return carry

    lax.fori_loop(0, PEERS, angle_tables, 0)

    arrived(VOLUME)
    v_twin.start()
    copy(v_all.at[:, 1 - core], v_all.at[:, 1 - core], one_ss.at[0], one_rs.at[0], twin).wait_recv()
    xs[...] = dot(v_all[...].reshape(N, N), tab_ref[FWD_X])

    def turned(p_part, q_part, table, p, rows, sign):
        cos, sin, end = table[p, 0, rows], table[p, 1, rows], table[p, 2, rows]
        if sign > 0:
            return p_part * cos + q_part * sin, q_part * end - p_part * sin
        return p_part * cos - q_part * sin, q_part * end + p_part * sin

    whole = slice(None)

    def sheared(prepare, start, middle, sign):
        for i, part in enumerate(parts):
            prepare(i, part)
            for j, p in enumerate(order):
                for r in range(part.start, part.stop, STRIP):
                    rows = slice(r, r + STRIP)
                    first, second = start(j, rows)
                    first, second = turned(first, second, tab_a, p, rows, sign)
                    work_a[j, rows, :HALF] = first.astype(BF16)
                    work_a[j, rows, HALF:] = second.astype(BF16)
        middle()
        for j in range(PEERS):
            work_b[j] = dot(work_a[j], tab_ref[INV_X]).astype(BF16)
        for j, p in enumerate(order):
            y = dot(tab_ref[FWD_Y], work_b[j])
            first, second = turned(y[:HALF], y[HALF:], tab_b, p, whole, sign)
            work_a[j, :HALF] = first.astype(BF16)
            work_a[j, HALF:] = second.astype(BF16)
        for j in range(PEERS):
            work_b[j] = dot(tab_ref[INV_Y], work_a[j]).astype(BF16)

    def projected(prepare, middle):
        sheared(prepare, lambda j, rows: (xs[rows, :HALF], xs[rows, HALF:]), middle, 1)
        spectra = []
        for j, p in enumerate(order):
            y = dot(work_b[j], tab_ref[FWD_X])
            turn = turned(y[:, :HALF], y[:, HALF:], tab_a, p, whole, 1)
            spectra.append(jnp.sum(jnp.concatenate(turn, axis=1), axis=0, keepdims=True))
        return dot_parts(jnp.concatenate(spectra, axis=0), tab_ref[INV_X]) * (1.0 / math.sqrt(N))

    def nothing(*unused):
        pass

    arrived(GRAD)
    grad = jnp.sum(g_all[...].astype(F32), axis=0)
    base = phase_ref[...] - eta_step * (grad + dual_ref[...] + rho_weight * phase_ref[...])
    lines = rho_weight * base + dual_ref[...]
    for q in range(PEERS):
        l_send[q] = lines[q : q + 1]
    for p in range(PEERS):
        l_copy(p, mine).start()

    arrived(SMOOTH)
    b_twin.start()
    old = projected(nothing, nothing)
    for j, p in enumerate(order):
        old_send[j] = old[j : j + 1]
    for j, p in enumerate(order):
        old_copy(j, p, my_slot).start()
    copy(b_all.at[:, 1 - core], b_all.at[:, 1 - core], one_ss.at[1], one_rs.at[1], twin).wait_recv()
    xb[...] = dot(b_all[...].reshape(N, N), tab_ref[FWD_X])

    arrived(LINES)
    asked = jnp.concatenate([l_all[p] for p in order], axis=0)
    resid = (rho_weight * (1.0 - eta_step * rho_weight)) * old - asked
    asked = dot_parts(resid, tab_ref[FWD_X]) * (1.0 / math.sqrt(N))
    sheared(nothing, lambda j, rows: (asked[j : j + 1, :HALF], asked[j : j + 1, HALF:]), nothing, -1)
    size = N // PARTS
    for i, rows in enumerate(parts):
        y = dot(work_b[:, rows].reshape(PEERS * size, N), tab_ref[FWD_X])
        total = jnp.zeros((size, N), F32)
        for j, p in enumerate(order):
            here = y[j * size : (j + 1) * size]
            total = total + jnp.concatenate(turned(here[:, :HALF], here[:, HALF:], tab_a, p, rows, -1), axis=1)
        s_sum[rows] = total
        s_send[rows] = total.astype(BF16)
        s_twins[i].start()

    def take_twin(i, rows):
        s_twins[i].wait_recv()
        total = s_sum[rows] + s_recv[rows].astype(F32)
        s_sum[rows] = total
        xs[rows] = xb[rows] - tau_step * total

    def send_back():
        blocks = s_sum[...].astype(BF16).reshape(PEERS, 2, ROWS, N)
        blocks = jnp.where(core == 0, blocks[:, 0], blocks[:, 1]).reshape(HALF, N)
        k_send[...] = dot(blocks, tab_ref[INV_X]).astype(BF16).reshape(PEERS, ROWS, N)
        for p in range(PEERS):
            k_copy(p, my_slot).start()

    new = projected(take_twin, send_back)
    for j, p in enumerate(order):
        new_send[j] = new[j : j + 1]
    for j, p in enumerate(order):
        new_copy(j, p, my_slot).start()

    arrived(BACK)
    for q in range(PEERS):
        vol_made[:, q, :] = b_own[q] - tau_step * k_all[q].astype(F32)
    leave_vol = pltpu.make_async_copy(vol_made, vol_out, in_sem.at[0])
    leave_phase = pltpu.make_async_copy(phase_made, phase_out, in_sem.at[1])
    leave_dual = pltpu.make_async_copy(dual_made, dual_out, in_sem.at[2])
    leave_vol.start()
    arrived(OLD)
    phase_new = base + (eta_step * rho_weight) * jnp.concatenate([old_all[q] for q in range(PEERS)], axis=0)
    phase_made[...] = phase_new
    leave_phase.start()
    arrived(NEW)
    after = jnp.concatenate([new_all[q] for q in range(PEERS)], axis=0)
    dual_made[...] = dual_ref[...] + rho_weight * (phase_new - after)
    leave_dual.start()

    for i, group in enumerate(groups):
        copy(group, group, sent.at[i], came.at[i], twin).wait_send()
    for one in [v_twin, b_twin, halo_up, halo_down] + s_twins:
        one.wait_send()
    for leave in (leave_vol, leave_phase, leave_dual):
        leave.wait()


def hand_over(phase_in, vol_in, dual_in, phase_out, vol_out, dual_out):
    phase_out[...] = phase_in[...]
    vol_out[...] = vol_in[...]
    dual_out[...] = dual_in[...]


def shards(volume, phase, dual, probe_real, probe_imag, intensity, offsets, angle_index):
    tables = jnp.asarray(packed_tables()).astype(BF16)
    in_vmem = pl.BlockSpec(memory_space=pltpu.VMEM)
    in_place = pl.BlockSpec(memory_space=pltpu.HBM)
    dma = pltpu.SemaphoreType.DMA
    vmem = pltpu.VMEM
    blocks = (PEERS, ROWS, N)
    lines = (PEERS, 1, N)
    results = (
        jax.ShapeDtypeStruct(phase.shape[1:], F32),
        jax.ShapeDtypeStruct(volume.shape, F32),
        jax.ShapeDtypeStruct(dual.shape[1:], F32),
    )
    made = pl.pallas_call(
        step_kernel,
        out_shape=results,
        in_specs=[in_place] * 9,
        out_specs=(in_place,) * 3,
        scratch_shapes=[
            pltpu.SMEM((1, SHOTS), jnp.int32),
            pltpu.SMEM((1,), jnp.int32),
            vmem(volume.shape, F32),
            vmem((8, N), F32),
            vmem((8, N), F32),
            vmem((HALF, HALF), F32),
            vmem((HALF, HALF), F32),
            vmem((SHOTS, HALF, HALF), F32),
            vmem(tables.shape, BF16),
            vmem((8, N), BF16),
            vmem((8, 128), F32),
            vmem((PEERS, 8, 128), F32),
            vmem(blocks, BF16),
            vmem((PEERS, 2, ROWS, N), BF16),
            vmem(blocks, BF16),
            vmem((PEERS, 2, ROWS, N), BF16),
            vmem(blocks, F32),
            vmem((2, ROWS, N), BF16),
            vmem((TILES, 8, N), BF16),
            vmem((TILES, 8, N), BF16),
            vmem((TILES, 8, N), BF16),
            vmem(lines, F32),
            vmem(lines, F32),
            vmem(lines, F32),
            vmem(lines, F32),
            vmem(lines, F32),
            vmem(lines, F32),
            vmem(blocks, BF16),
            vmem(blocks, BF16),
            vmem((N, N), BF16),
            vmem((N, N), BF16),
            vmem((PEERS, N, N), BF16),
            vmem((PEERS, N, N), BF16),
            vmem(volume.shape, F32),
            vmem((8, N), F32),
            vmem((8, N), F32),
            vmem((PEERS, 3, N, HALF), F32),
            vmem((PEERS, 3, HALF, N), F32),
            vmem((N, N), F32),
            vmem((N, N), F32),
            vmem((N, N), F32),
            vmem((SHOTS, 2, HALF, HALF), F32),
            dma((9,)),
            dma((9,)),
            dma((4,)),
            dma((4,)),
            dma((PARTS,)),
            dma((PARTS,)),
            dma((9,)),
        ],
        compiler_params=pltpu.CompilerParams(collective_id=0, has_side_effects=True),
    )(offsets, angle_index, volume, phase[0], dual[0], probe_real, probe_imag, intensity[0], tables)
    phase_new, volume_new, dual_new = pl.pallas_call(
        hand_over, out_shape=results, in_specs=[in_vmem] * 3, out_specs=(in_vmem,) * 3
    )(*made)
    return (phase_new[None], volume_new, dual_new[None])


def solution(mesh):
    placed = (
        P("ang", "tile", None),
        P("ang", "tile", None),
        P("ang", "tile", None),
        P(),
        P(),
        P("ang", "tile", None, None),
        P("ang", "tile"),
        P("ang"),
    )
    return jax.shard_map(
        shards,
        mesh=mesh,
        in_specs=placed,
        out_specs=(P("ang", "tile", None), P("ang", "tile", None), P("ang", "tile", None)),
        check_vma=False,
    )
```

```python
import math

import jax
import jax.numpy as jnp
import numpy as np
from jax import lax
from jax.experimental import pallas as pl
from jax.experimental.pallas import tpu as pltpu
from jax.sharding import PartitionSpec as P

angle_center = 90.0
rho_weight = 1.0
eta_step = 0.01
tau_step = 1.0
smooth_weight = 0.25

N = 256
HALF = 128
PEERS = 8
TILES = 16
ROWS = 16
SHOTS = 4
BAND_ROWS = 128
STRIP = 32
FWD_X, INV_X, FWD_Y, INV_Y = range(4)
PHASE, GRAD, COEF, VOLUME, SMOOTH, LINES, OLD, NEW, BACK = range(9)
PARTS = 2
NEAR_LAST = [4 * dy + dz for dy in (2, 1, 3, 0) for dz in range(4) if dy or dz]
F32 = jnp.float32
BF16 = jnp.bfloat16
MESH = pl.DeviceIdType.MESH


def tables_of(length):
    index = np.arange(length)
    phases = (index[:, None] * index[None, :] % length).astype(np.float32)
    phases = phases * np.float32(2.0 * math.pi / length)
    return np.cos(phases), np.sin(phases)


def packed_tables():
    cos, sin = tables_of(N)
    signs = np.where(np.arange(N) % 2 == 0, 1.0, -1.0)
    forward = np.concatenate([cos[:, :HALF], -sin[:, :HALF]], axis=1)
    forward[:, HALF] = signs
    inverse = np.concatenate([2.0 * cos[:HALF], -2.0 * sin[:HALF]], axis=0)
    inverse[0] = 1.0
    inverse[HALF] = signs
    inverse = inverse / N
    cos, sin = tables_of(HALF)
    cos, sin = cos / math.sqrt(HALF), sin / math.sqrt(HALF)
    near = np.block([[cos, -sin], [sin, cos]])
    away = np.block([[cos, sin], [-sin, cos]])
    stack = np.stack([forward, inverse, forward.T, inverse.T, near, away])
    return stack.astype(np.float32)


def sincos_turns(turns):
    a = (turns - jnp.floor(turns + 0.5)) * math.pi
    z = a * a
    sin = 1.0
    for k in (12, 10, 8, 6, 4, 2):
        sin = 1.0 - z * sin * (1.0 / (k * (k + 1)))
    sin = a * sin
    cos = 1.0
    for k in (13, 11, 9, 7, 5, 3, 1):
        cos = 1.0 - z * cos * (1.0 / (k * (k + 1)))
    return 2.0 * sin * cos, 1.0 - 2.0 * sin * sin


def dot(a, b):
    return jnp.dot(a, b, preferred_element_type=F32)


def two_parts(x):
    high = x.astype(BF16)
    low = (x - high.astype(F32)).astype(BF16)
    return jnp.concatenate([high, low], axis=0)


def dot_parts(x, table):
    both = dot(two_parts(x), table)
    return both[: x.shape[0]] + both[x.shape[0] :]


def step_kernel(
    offsets_in, angle_in, vol_in, phase_in, dual_in, pr_in, pi_in, inten_in, tab_in,
    phase_out, vol_out, dual_out,
    offsets_ref, angle_ref, vol_ref, phase_ref, dual_ref, pr_ref, pi_ref, inten_ref, tab_ref, phase_send,
    coef_send, coef_all, v_send, v_all, b_send, b_all, b_own, halo, phase_all, g_send, g_all, l_send, l_all,
    old_send, old_all, new_send, new_all, k_send, k_all, s_send, s_recv,
    work_a, work_b, vol_made, phase_made, dual_made, tab_a, tab_b, xs, xb, s_sum, wave,
    sent, came, one_ss, one_rs, part_ss, part_rs, in_sem,
):
    me = lax.axis_index("ang")
    tile = lax.axis_index("tile")
    core = me % 2
    mine = me // 2
    x_me, hi_me = mine // 2, mine % 2
    low = tile % 4
    far_tile = (tile // 4) * 4 + (low + 2) % 4
    turn_out = (low + 2) // 4
    turn_in = ((low + 2) % 4 + 2) // 4
    my_slot = 2 * x_me + (hi_me + turn_in) % 2
    twin = (me - core + (1 - core), tile)

    def peer(p):
        return (2 * p + core, far_tile)

    def slot_of(p):
        return 2 * (p // 2) + (p % 2 + turn_out) % 2

    def beside(o):
        return (me, ((tile // 4 + o // 4) % 4) * 4 + (low + o) % 4)

    order = [2 * ((x_me + dx) % 4) + zh for dx in (2, 1, 3, 0) for zh in (0, 1)]

    barrier = pltpu.get_barrier_semaphore()
    for o in NEAR_LAST:
        pl.semaphore_signal(barrier, inc=1, device_id=beside(o), device_id_type=MESH)
    for p in range(PEERS):
        pl.semaphore_signal(barrier, inc=1, device_id=peer(p), device_id_type=MESH)
    pl.semaphore_signal(barrier, inc=1, device_id=twin, device_id_type=MESH)

    loads = [
        pltpu.make_async_copy(src, dst, in_sem.at[i])
        for i, (src, dst) in enumerate(
            [
                (angle_in, angle_ref), (phase_in, phase_ref), (vol_in, vol_ref), (offsets_in, offsets_ref),
                (pr_in, pr_ref), (pi_in, pi_ref), (inten_in, inten_ref), (tab_in, tab_ref), (dual_in, dual_ref),
            ]
        )
    ]
    for load in loads:
        load.start()

    loads[0].wait()
    number = jnp.full((8, 128), angle_ref[0], jnp.int32).astype(F32) - angle_center
    sin_b, unused = sincos_turns(number * (1.0 / 720.0))
    sin_h, cos_h = sincos_turns(number * (1.0 / 1440.0))
    rows8 = lax.broadcasted_iota(jnp.int32, (8, 128), 0)
    coef_send[...] = jnp.where(rows8 < 4, -(sin_h / cos_h), sin_b)
    loads[1].wait()
    turns = phase_ref[...] * (1.0 / (2.0 * math.pi))
    phase_send[...] = (turns - jnp.floor(turns + 0.5)).astype(BF16)
    loads[2].wait()
    for q in range(PEERS):
        v_send[q] = vol_ref[:, q, :].astype(BF16)

    pl.semaphore_wait(barrier, TILES + PEERS)

    def copy(src, dst, send, recv, device):
        return pltpu.make_async_remote_copy(
            src_ref=src, dst_ref=dst, send_sem=send, recv_sem=recv, device_id=device, device_id_type=MESH
        )

    def phase_copy(o, slot):
        return copy(phase_send, phase_all.at[slot], sent.at[0], came.at[0], beside(o))

    def coef_copy(p, slot):
        return copy(coef_send, coef_all.at[slot], sent.at[2], came.at[2], peer(p))

    def v_copy(p, slot):
        return copy(v_send.at[slot_of(p)], v_all.at[slot, core], sent.at[3], came.at[3], peer(p))

    def b_copy(p, slot):
        return copy(b_send.at[slot_of(p)], b_all.at[slot, core], sent.at[4], came.at[4], peer(p))

    def g_copy(o, slot):
        return copy(g_send.at[beside(o)[1]], g_all.at[slot], sent.at[1], came.at[1], beside(o))

    def l_copy(p, slot):
        return copy(l_send.at[slot_of(p)], l_all.at[slot], sent.at[5], came.at[5], peer(p))

    def old_copy(j, p, slot):
        return copy(old_send.at[j], old_all.at[slot], sent.at[6], came.at[6], peer(p))

    def new_copy(j, p, slot):
        return copy(new_send.at[j], new_all.at[slot], sent.at[7], came.at[7], peer(p))

    def k_copy(p, slot):
        return copy(k_send.at[p], k_all.at[slot], sent.at[8], came.at[8], peer(p))

    others = pl.ds(0, TILES - 1)
    groups = [phase_all.at[others], g_all.at[others], coef_all, v_send, b_send, l_send, old_send, new_send, k_send]

    def arrived(group):
        copy(groups[group], groups[group], sent.at[group], came.at[group], twin).wait_recv()

    v_twin = copy(v_all.at[:, core], v_all.at[:, core], one_ss.at[0], one_rs.at[0], twin)
    b_twin = copy(b_all.at[:, core], b_all.at[:, core], one_ss.at[1], one_rs.at[1], twin)
    parts = [slice(r, r + N // PARTS) for r in range(0, N, N // PARTS)]
    s_twins = [
        copy(s_send.at[rows], s_recv.at[rows], part_ss.at[i], part_rs.at[i], twin) for i, rows in enumerate(parts)
    ]
    halo_up = copy(v_send.at[PEERS - 1], halo.at[0], one_ss.at[2], one_rs.at[2], (me, (tile + 1) % TILES))
    halo_down = copy(v_send.at[0], halo.at[1], one_ss.at[3], one_rs.at[3], (me, (tile + TILES - 1) % TILES))

    for o in NEAR_LAST:
        phase_copy(o, tile).start()
    for p in range(PEERS):
        coef_copy(p, mine).start()
    for p in range(PEERS):
        v_copy(p, mine).start()
    halo_up.start()
    halo_down.start()
    phase_all[tile] = phase_send[...]
    for load in loads[3:]:
        load.wait()
    near, away = tab_ref[4], tab_ref[5]

    arrived(PHASE)

    sin, cos = sincos_turns(phase_all[...].astype(F32).reshape(BAND_ROWS, N))
    waves = []
    for s in range(SHOTS):
        back = (N - offsets_ref[0, s]) % N
        c, n = pltpu.roll(cos, back, 1)[:, :HALF], pltpu.roll(sin, back, 1)[:, :HALF]
        wave_r = pr_ref[...] * c - pi_ref[...] * n
        wave_i = pr_ref[...] * n + pi_ref[...] * c
        wave[s, 0] = wave_r
        wave[s, 1] = wave_i
        waves.append(jnp.concatenate([wave_r, wave_i], axis=1).astype(BF16))
    half = dot(jnp.concatenate(waves, axis=0), near).astype(BF16)
    beams = [half[s * HALF : (s + 1) * HALF] for s in range(SHOTS)]
    beams = [jnp.concatenate([b[:, :HALF], b[:, HALF:]], axis=0) for b in beams]
    far = dot(away, jnp.concatenate(beams, axis=1))
    far_r, far_i = far[:HALF], far[HALF:]
    measured = jnp.concatenate([inten_ref[s] for s in range(SHOTS)], axis=1)
    misfit = far_r * far_r + far_i * far_i - measured
    weighted = jnp.concatenate([misfit * far_r, misfit * far_i], axis=0).astype(BF16)
    half = dot(near, weighted).astype(BF16)
    beams = [half[:, s * HALF : (s + 1) * HALF] for s in range(SHOTS)]
    beams = [jnp.concatenate([b[:HALF], b[HALF:]], axis=1) for b in beams]
    leave = dot(jnp.concatenate(beams, axis=0), away)
    image = jnp.zeros((BAND_ROWS, N), F32)
    for s in range(SHOTS):
        e = leave[s * HALF : (s + 1) * HALF]
        term = 2.0 * (e[:, HALF:] * wave[s, 0] - e[:, :HALF] * wave[s, 1])
        wide = jnp.concatenate([term, jnp.zeros((BAND_ROWS, N - HALF), F32)], axis=1)
        image = image + pltpu.roll(wide, offsets_ref[0, s], 1)
    g_send[...] = image.reshape(TILES, 8, N).astype(BF16)
    for o in NEAR_LAST:
        g_copy(o, tile).start()
    g_all[tile] = g_send[tile]
    halo_up.wait_recv()
    halo_down.wait_recv()
    lower = jnp.where(tile > 0, halo[0].astype(F32), 0.0)
    upper = jnp.where(tile < TILES - 1, halo[1].astype(F32), 0.0)
    for q in range(PEERS):
        here = vol_ref[:, q, :]
        before = lower if q == 0 else vol_ref[:, q - 1, :]
        after = upper if q == PEERS - 1 else vol_ref[:, q + 1, :]
        value = here - (tau_step * smooth_weight) * (2.0 * here - before - after)
        b_own[q] = value
        b_send[q] = value.astype(BF16)
    for p in range(PEERS):
        b_copy(p, mine).start()

    arrived(COEF)

    lane = lax.broadcasted_iota(jnp.int32, (N, HALF), 1)
    line = lax.broadcasted_iota(jnp.int32, (N, HALF), 0)
    freq_a = jnp.where(lane == 0, HALF, lane).astype(F32) * (1.0 / N)
    row_a = (line - HALF).astype(F32)
    lane_b = lax.broadcasted_iota(jnp.int32, (HALF, N), 1)
    line_b = lax.broadcasted_iota(jnp.int32, (HALF, N), 0)
    freq_b = jnp.where(line_b == 0, HALF, line_b).astype(F32) * (1.0 / N)
    row_b = (lane_b - HALF).astype(F32)

    def angle_tables(p, carry):
        coef = coef_all[p]
        shift = coef[0:1, :]
        sin, cos = sincos_turns((row_a * shift) * freq_a)
        tab_a[p, 0] = jnp.where(lane == 0, 1.0, cos)
        tab_a[p, 1] = jnp.where(lane == 0, 0.0, sin)
        tab_a[p, 2] = cos
        shift = jnp.concatenate([coef[4:5, :], coef[4:5, :]], axis=1)
        sin, cos = sincos_turns((row_b * shift) * freq_b)
        tab_b[p, 0] = jnp.where(line_b == 0, 1.0, cos)
        tab_b[p, 1] = jnp.where(line_b == 0, 0.0, sin)
        tab_b[p, 2] = cos
        return carry

    lax.fori_loop(0, PEERS, angle_tables, 0)

    arrived(VOLUME)
    v_twin.start()
    def turned(p_part, q_part, table, p, rows, sign):
        cos, sin, end = table[p, 0, rows], table[p, 1, rows], table[p, 2, rows]
        if sign > 0:
            return p_part * cos + q_part * sin, q_part * end - p_part * sin
        return p_part * cos - q_part * sin, q_part * end + p_part * sin

    whole = slice(None)

    def sheared(prepare, start, middle, sign):
        for i, part in enumerate(parts):
            prepare(i, part)
            for j, p in enumerate(order):
                for r in range(part.start, part.stop, STRIP):
                    rows = slice(r, r + STRIP)
                    first, second = start(j, rows)
                    first, second = turned(first, second, tab_a, p, rows, sign)
                    work_a[j, rows, :HALF] = first.astype(BF16)
                    work_a[j, rows, HALF:] = second.astype(BF16)
        middle()
        for j in range(PEERS):
            work_b[j] = dot(work_a[j], tab_ref[INV_X]).astype(BF16)
        for j, p in enumerate(order):
            y = dot(tab_ref[FWD_Y], work_b[j])
            first, second = turned(y[:HALF], y[HALF:], tab_b, p, whole, sign)
            work_a[j, :HALF] = first.astype(BF16)
            work_a[j, HALF:] = second.astype(BF16)
        for j in range(PEERS):
            work_b[j] = dot(tab_ref[INV_Y], work_a[j]).astype(BF16)

    def projected(prepare, middle, groups, finish):
        sheared(prepare, lambda j, rows: (xs[rows, :HALF], xs[rows, HALF:]), middle, 1)
        for js in groups:
            spectra = []
            for j in js:
                y = dot(work_b[j], tab_ref[FWD_X])
                turn = turned(y[:, :HALF], y[:, HALF:], tab_a, order[j], whole, 1)
                spectra.append(jnp.sum(jnp.concatenate(turn, axis=1), axis=0, keepdims=True))
            finish(js, dot_parts(jnp.concatenate(spectra, axis=0), tab_ref[INV_X]) * (1.0 / math.sqrt(N)))

    def nothing(*unused):
        pass

    arrived(GRAD)
    grad = jnp.sum(g_all[...].astype(F32), axis=0)
    base = phase_ref[...] - eta_step * (grad + dual_ref[...] + rho_weight * phase_ref[...])
    lines = rho_weight * base + dual_ref[...]
    for q in range(PEERS):
        l_send[q] = lines[q : q + 1]
    for p in range(PEERS):
        l_copy(p, mine).start()

    copy(v_all.at[:, 1 - core], v_all.at[:, 1 - core], one_ss.at[0], one_rs.at[0], twin).wait_recv()
    xs[...] = dot(v_all[...].reshape(N, N), tab_ref[FWD_X])

    arrived(SMOOTH)
    b_twin.start()
    kept = []

    def send_old(js, lines):
        kept.append(lines)
        for j in js:
            old_send[j] = lines[j : j + 1]
        for j in js:
            old_copy(j, order[j], my_slot).start()

    projected(nothing, nothing, [range(PEERS)], send_old)
    old = kept[0]
    copy(b_all.at[:, 1 - core], b_all.at[:, 1 - core], one_ss.at[1], one_rs.at[1], twin).wait_recv()
    xb[...] = dot(b_all[...].reshape(N, N), tab_ref[FWD_X])

    arrived(LINES)
    asked = jnp.concatenate([l_all[p] for p in order], axis=0)
    resid = (rho_weight * (1.0 - eta_step * rho_weight)) * old - asked
    asked = dot_parts(resid, tab_ref[FWD_X]) * (1.0 / math.sqrt(N))
    sheared(nothing, lambda j, rows: (asked[j : j + 1, :HALF], asked[j : j + 1, HALF:]), nothing, -1)
    for j, p in enumerate(order[:-1]):
        y = dot(work_b[j], tab_ref[FWD_X])
        turn = jnp.concatenate(turned(y[:, :HALF], y[:, HALF:], tab_a, p, whole, -1), axis=1)
        s_sum[...] = turn if j == 0 else s_sum[...] + turn
    for i, rows in enumerate(parts):
        y = dot(work_b[PEERS - 1, rows], tab_ref[FWD_X])
        turn = turned(y[:, :HALF], y[:, HALF:], tab_a, order[-1], rows, -1)
        total = s_sum[rows] + jnp.concatenate(turn, axis=1)
        s_sum[rows] = total
        s_send[rows] = total.astype(BF16)
        s_twins[i].start()

    def take_twin(i, rows):
        s_twins[i].wait_recv()
        total = s_sum[rows] + s_recv[rows].astype(F32)
        s_sum[rows] = total
        xs[rows] = xb[rows] - tau_step * total

    def send_back():
        blocks = s_sum[...].astype(BF16).reshape(PEERS, 2, ROWS, N)
        blocks = jnp.where(core == 0, blocks[:, 0], blocks[:, 1]).reshape(HALF, N)
        k_send[...] = dot(blocks, tab_ref[INV_X]).astype(BF16).reshape(PEERS, ROWS, N)
        for p in range(PEERS):
            k_copy(p, my_slot).start()

    def send_new(js, lines):
        for j in js:
            new_send[j] = lines[j - js[0] : j - js[0] + 1]
        for j in js:
            new_copy(j, order[j], my_slot).start()

    projected(take_twin, send_back, [range(2), range(2, PEERS)], send_new)

    arrived(BACK)
    for q in range(PEERS):
        vol_out[:, q, :] = b_own[q] - tau_step * k_all[q].astype(F32)
    arrived(OLD)
    phase_new = base + (eta_step * rho_weight) * jnp.concatenate([old_all[q] for q in range(PEERS)], axis=0)
    phase_out[...] = phase_new
    arrived(NEW)
    after = jnp.concatenate([new_all[q] for q in range(PEERS)], axis=0)
    dual_out[...] = dual_ref[...] + rho_weight * (phase_new - after)

    for i, group in enumerate(groups):
        copy(group, group, sent.at[i], came.at[i], twin).wait_send()
    for one in [v_twin, b_twin, halo_up, halo_down] + s_twins:
        one.wait_send()


def hand_over(phase_in, vol_in, dual_in, phase_out, vol_out, dual_out):
    phase_out[...] = phase_in[...]
    vol_out[...] = vol_in[...]
    dual_out[...] = dual_in[...]


def shards(volume, phase, dual, probe_real, probe_imag, intensity, offsets, angle_index):
    tables = jnp.asarray(packed_tables()).astype(BF16)
    in_vmem = pl.BlockSpec(memory_space=pltpu.VMEM)
    in_place = pl.BlockSpec(memory_space=pltpu.HBM)
    dma = pltpu.SemaphoreType.DMA
    vmem = pltpu.VMEM
    blocks = (PEERS, ROWS, N)
    lines = (PEERS, 1, N)
    results = (
        jax.ShapeDtypeStruct(phase.shape[1:], F32),
        jax.ShapeDtypeStruct(volume.shape, F32),
        jax.ShapeDtypeStruct(dual.shape[1:], F32),
    )
    made = pl.pallas_call(
        step_kernel,
        out_shape=results,
        in_specs=[in_place] * 9,
        out_specs=(in_vmem,) * 3,
        scratch_shapes=[
            pltpu.SMEM((1, SHOTS), jnp.int32),
            pltpu.SMEM((1,), jnp.int32),
            vmem(volume.shape, F32),
            vmem((8, N), F32),
            vmem((8, N), F32),
            vmem((HALF, HALF), F32),
            vmem((HALF, HALF), F32),
            vmem((SHOTS, HALF, HALF), F32),
            vmem(tables.shape, BF16),
            vmem((8, N), BF16),
            vmem((8, 128), F32),
            vmem((PEERS, 8, 128), F32),
            vmem(blocks, BF16),
            vmem((PEERS, 2, ROWS, N), BF16),
            vmem(blocks, BF16),
            vmem((PEERS, 2, ROWS, N), BF16),
            vmem(blocks, F32),
            vmem((2, ROWS, N), BF16),
            vmem((TILES, 8, N), BF16),
            vmem((TILES, 8, N), BF16),
            vmem((TILES, 8, N), BF16),
            vmem(lines, F32),
            vmem(lines, F32),
            vmem(lines, F32),
            vmem(lines, F32),
            vmem(lines, F32),
            vmem(lines, F32),
            vmem(blocks, BF16),
            vmem(blocks, BF16),
            vmem((N, N), BF16),
            vmem((N, N), BF16),
            vmem((PEERS, N, N), BF16),
            vmem((PEERS, N, N), BF16),
            vmem(volume.shape, F32),
            vmem((8, N), F32),
            vmem((8, N), F32),
            vmem((PEERS, 3, N, HALF), F32),
            vmem((PEERS, 3, HALF, N), F32),
            vmem((N, N), F32),
            vmem((N, N), F32),
            vmem((N, N), F32),
            vmem((SHOTS, 2, HALF, HALF), F32),
            dma((9,)),
            dma((9,)),
            dma((4,)),
            dma((4,)),
            dma((PARTS,)),
            dma((PARTS,)),
            dma((9,)),
        ],
        compiler_params=pltpu.CompilerParams(collective_id=0, has_side_effects=True, vmem_limit_bytes=24 << 20),
    )(*[pltpu.with_memory_space_constraint(x, pltpu.HBM) for x in (offsets,)], angle_index, *[pltpu.with_memory_space_constraint(x, pltpu.HBM) for x in (volume, phase[0], dual[0], probe_real, probe_imag, intensity[0], tables)])
    phase_new, volume_new, dual_new = pl.pallas_call(
        hand_over, out_shape=results, in_specs=[in_vmem] * 3, out_specs=(in_vmem,) * 3, compiler_params=pltpu.CompilerParams(vmem_limit_bytes=4 << 20)
    )(*made)
    return (phase_new[None], volume_new, dual_new[None])


def solution(mesh):
    placed = (
        P("ang", "tile", None),
        P("ang", "tile", None),
        P("ang", "tile", None),
        P(),
        P(),
        P("ang", "tile", None, None),
        P("ang", "tile"),
        P("ang"),
    )
    return jax.shard_map(
        shards,
        mesh=mesh,
        in_specs=placed,
        out_specs=(P("ang", "tile", None), P("ang", "tile", None), P("ang", "tile", None)),
        check_vma=False,
    )
```

```python
import math

import jax
import jax.numpy as jnp
import numpy as np
from jax import lax
from jax.experimental import pallas as pl
from jax.experimental.pallas import tpu as pltpu
from jax.sharding import PartitionSpec as P

angle_center = 90.0
rho_weight = 1.0
eta_step = 0.01
tau_step = 1.0
smooth_weight = 0.25

N = 256
HALF = 128
PEERS = 8
TILES = 16
ROWS = 16
SHOTS = 4
BAND_ROWS = 128
STRIP = 32
FWD_X, INV_X, FWD_Y, INV_Y = range(4)
PHASE, GRAD, COEF, VOLUME, SMOOTH, LINES, OLD, NEW, BACK = range(9)
PARTS = 2
AWAY = [2, 2, 1, 1, 1, 1, 0, 0]
MOVED = (0, 1, 4, 5)
LATE = 4
NEAR_LAST = [4 * dy + dz for dy in (2, 1, 3, 0) for dz in range(4) if dy or dz]
F32 = jnp.float32
BF16 = jnp.bfloat16
MESH = pl.DeviceIdType.MESH


def tables_of(length):
    index = np.arange(length)
    phases = (index[:, None] * index[None, :] % length).astype(np.float32)
    phases = phases * np.float32(2.0 * math.pi / length)
    return np.cos(phases), np.sin(phases)


def packed_tables():
    cos, sin = tables_of(N)
    signs = np.where(np.arange(N) % 2 == 0, 1.0, -1.0)
    forward = np.concatenate([cos[:, :HALF], -sin[:, :HALF]], axis=1)
    forward[:, HALF] = signs
    inverse = np.concatenate([2.0 * cos[:HALF], -2.0 * sin[:HALF]], axis=0)
    inverse[0] = 1.0
    inverse[HALF] = signs
    inverse = inverse / N
    cos, sin = tables_of(HALF)
    cos, sin = cos / math.sqrt(HALF), sin / math.sqrt(HALF)
    near = np.block([[cos, -sin], [sin, cos]])
    away = np.block([[cos, sin], [-sin, cos]])
    stack = np.stack([forward, inverse, forward.T, inverse.T, near, away])
    return stack.astype(np.float32)


def sincos_turns(turns):
    a = (turns - jnp.floor(turns + 0.5)) * math.pi
    z = a * a
    sin = 1.0
    for k in (12, 10, 8, 6, 4, 2):
        sin = 1.0 - z * sin * (1.0 / (k * (k + 1)))
    sin = a * sin
    cos = 1.0
    for k in (13, 11, 9, 7, 5, 3, 1):
        cos = 1.0 - z * cos * (1.0 / (k * (k + 1)))
    return 2.0 * sin * cos, 1.0 - 2.0 * sin * sin


def dot(a, b):
    return jnp.dot(a, b, preferred_element_type=F32)


def two_parts(x):
    high = x.astype(BF16)
    low = (x - high.astype(F32)).astype(BF16)
    return jnp.concatenate([high, low], axis=0)


def dot_parts(x, table):
    both = dot(two_parts(x), table)
    return both[: x.shape[0]] + both[x.shape[0] :]


def step_kernel(
    offsets_in, angle_in, vol_in, phase_in, dual_in, pr_in, pi_in, inten_in, tab_in,
    phase_out, vol_out, dual_out,
    offsets_ref, angle_ref, vol_ref, phase_ref, dual_ref, pr_ref, pi_ref, inten_ref, tab_ref, phase_send,
    coef_send, coef_all, coef_other, v_send, v_all, b_send, b_all, b_own, halo, phase_all, g_send, g_all, l_send, l_all,
    old_send, old_all, new_send, new_all, k_send, k_all, s_send, s_recv,
    work_a, work_b, vol_made, phase_made, dual_made, tab_a, tab_b, xs, xb, s_sum, wave,
    sent, came, near_rs, one_ss, one_rs, part_ss, part_rs, in_sem,
):
    me = lax.axis_index("ang")
    tile = lax.axis_index("tile")
    core = me % 2
    mine = me // 2
    x_me, hi_me = mine // 2, mine % 2
    low = tile % 4
    far_tile = (tile // 4) * 4 + (low + 2) % 4
    turn_out = (low + 2) // 4
    turn_in = ((low + 2) % 4 + 2) // 4
    my_slot = 2 * x_me + (hi_me + turn_in) % 2
    twin = (me - core + (1 - core), tile)

    def peer(p):
        return (2 * p + core, far_tile)

    def slot_of(p):
        return 2 * (p // 2) + (p % 2 + turn_out) % 2

    def beside(o):
        return (me, ((tile // 4 + o // 4) % 4) * 4 + (low + o) % 4)

    order = [2 * ((x_me + dx) % 4) + zh for dx in (2, 1, 3, 0) for zh in (0, 1)]

    barrier = pltpu.get_barrier_semaphore()
    for o in NEAR_LAST:
        pl.semaphore_signal(barrier, inc=1, device_id=beside(o), device_id_type=MESH)
    for p in range(PEERS):
        pl.semaphore_signal(barrier, inc=1, device_id=peer(p), device_id_type=MESH)
    for p in range(PEERS):
        pl.semaphore_signal(barrier, inc=1, device_id=(2 * p + 1 - core, far_tile), device_id_type=MESH)
    pl.semaphore_signal(barrier, inc=1, device_id=twin, device_id_type=MESH)

    loads = [
        pltpu.make_async_copy(src, dst, in_sem.at[i])
        for i, (src, dst) in enumerate(
            [
                (angle_in, angle_ref), (phase_in, phase_ref), (vol_in, vol_ref), (offsets_in, offsets_ref),
                (pr_in, pr_ref), (pi_in, pi_ref), (inten_in, inten_ref), (tab_in, tab_ref), (dual_in, dual_ref),
            ]
        )
    ]
    for load in loads:
        load.start()

    loads[0].wait()
    number = jnp.full((8, 128), angle_ref[0], jnp.int32).astype(F32) - angle_center
    sin_b, unused = sincos_turns(number * (1.0 / 720.0))
    sin_h, cos_h = sincos_turns(number * (1.0 / 1440.0))
    rows8 = lax.broadcasted_iota(jnp.int32, (8, 128), 0)
    coef_send[...] = jnp.where(rows8 < 4, -(sin_h / cos_h), sin_b)
    loads[1].wait()
    turns = phase_ref[...] * (1.0 / (2.0 * math.pi))
    phase_send[...] = (turns - jnp.floor(turns + 0.5)).astype(BF16)
    loads[2].wait()
    for q in range(PEERS):
        v_send[q] = vol_ref[:, q, :].astype(BF16)

    pl.semaphore_wait(barrier, TILES + 2 * PEERS)

    def copy(src, dst, send, recv, device):
        return pltpu.make_async_remote_copy(
            src_ref=src, dst_ref=dst, send_sem=send, recv_sem=recv, device_id=device, device_id_type=MESH
        )

    def phase_copy(o, slot):
        return copy(phase_send, phase_all.at[slot], sent.at[0], came.at[0], beside(o))

    def coef_copy(p, slot):
        return copy(coef_send, coef_all.at[slot], sent.at[2], came.at[2], peer(p))

    def v_copy(p, slot):
        return copy(v_send.at[slot_of(p)], v_all.at[slot, core], sent.at[3], came.at[3], peer(p))

    def b_copy(p, slot):
        return copy(b_send.at[slot_of(p)], b_all.at[slot, core], sent.at[4], came.at[4], peer(p))

    def g_copy(o, slot):
        return copy(g_send.at[beside(o)[1]], g_all.at[slot], sent.at[1], came.at[1], beside(o))

    def l_copy(j, p, slot):
        if j in MOVED:
            row, came_at = slot + PEERS * (1 - core), jnp.where(core == 1, AWAY[j], 3)
            return copy(l_send.at[slot_of(p)], l_all.at[row], sent.at[5], near_rs.at[came_at], (2 * p + 1, far_tile))
        return copy(l_send.at[slot_of(p)], l_all.at[slot], sent.at[5], near_rs.at[AWAY[j]], peer(p))

    def old_copy(j, p, slot):
        return copy(old_send.at[j], old_all.at[slot], sent.at[6], came.at[6], peer(p))

    def new_copy(j, p, slot):
        return copy(new_send.at[j], new_all.at[slot], sent.at[7], came.at[7], peer(p))

    def k_copy(p, slot):
        return copy(k_send.at[p], k_all.at[slot], sent.at[8], came.at[8], peer(p))

    others = pl.ds(0, TILES - 1)
    groups = [phase_all.at[others], g_all.at[others], coef_all, v_send, b_send, l_send, old_all, new_send, k_send]

    def arrived(group):
        copy(groups[group], groups[group], sent.at[group], came.at[group], twin).wait_recv()

    v_twin = copy(v_all.at[:, core], v_all.at[:, core], one_ss.at[0], one_rs.at[0], twin)
    b_twin = copy(b_all.at[:, core], b_all.at[:, core], one_ss.at[1], one_rs.at[1], twin)
    parts = [slice(r, r + N // PARTS) for r in range(0, N, N // PARTS)]
    s_twins = [
        copy(s_send.at[rows], s_recv.at[rows], part_ss.at[i], part_rs.at[i], twin) for i, rows in enumerate(parts)
    ]
    coef_twin = copy(coef_all, coef_other, one_ss.at[4], one_rs.at[4], twin)
    old_twin = copy(old_send.at[pl.ds(0, PEERS)], old_send.at[pl.ds(PEERS, PEERS)], one_ss.at[5], one_rs.at[5], twin)
    halo_up = copy(v_send.at[PEERS - 1], halo.at[0], one_ss.at[2], one_rs.at[2], (me, (tile + 1) % TILES))
    halo_down = copy(v_send.at[0], halo.at[1], one_ss.at[3], one_rs.at[3], (me, (tile + TILES - 1) % TILES))

    for o in NEAR_LAST:
        phase_copy(o, tile).start()
    for p in range(PEERS):
        coef_copy(p, mine).start()
    for p in range(PEERS):
        v_copy(p, mine).start()
    halo_up.start()
    halo_down.start()
    phase_all[tile] = phase_send[...]
    for load in loads[3:]:
        load.wait()
    near, away = tab_ref[4], tab_ref[5]

    arrived(PHASE)

    sin, cos = sincos_turns(phase_all[...].astype(F32).reshape(BAND_ROWS, N))
    waves = []
    for s in range(SHOTS):
        back = (N - offsets_ref[0, s]) % N
        c, n = pltpu.roll(cos, back, 1)[:, :HALF], pltpu.roll(sin, back, 1)[:, :HALF]
        wave_r = pr_ref[...] * c - pi_ref[...] * n
        wave_i = pr_ref[...] * n + pi_ref[...] * c
        wave[s, 0] = wave_r
        wave[s, 1] = wave_i
        waves.append(jnp.concatenate([wave_r, wave_i], axis=1).astype(BF16))
    half = dot(jnp.concatenate(waves, axis=0), near).astype(BF16)
    beams = [half[s * HALF : (s + 1) * HALF] for s in range(SHOTS)]
    beams = [jnp.concatenate([b[:, :HALF], b[:, HALF:]], axis=0) for b in beams]
    far = dot(away, jnp.concatenate(beams, axis=1))
    far_r, far_i = far[:HALF], far[HALF:]
    measured = jnp.concatenate([inten_ref[s] for s in range(SHOTS)], axis=1)
    misfit = far_r * far_r + far_i * far_i - measured
    weighted = jnp.concatenate([misfit * far_r, misfit * far_i], axis=0).astype(BF16)
    half = dot(near, weighted).astype(BF16)
    beams = [half[:, s * HALF : (s + 1) * HALF] for s in range(SHOTS)]
    beams = [jnp.concatenate([b[:HALF], b[HALF:]], axis=1) for b in beams]
    leave = dot(jnp.concatenate(beams, axis=0), away)
    image = jnp.zeros((BAND_ROWS, N), F32)
    for s in range(SHOTS):
        e = leave[s * HALF : (s + 1) * HALF]
        term = 2.0 * (e[:, HALF:] * wave[s, 0] - e[:, :HALF] * wave[s, 1])
        wide = jnp.concatenate([term, jnp.zeros((BAND_ROWS, N - HALF), F32)], axis=1)
        image = image + pltpu.roll(wide, offsets_ref[0, s], 1)
    g_send[...] = image.reshape(TILES, 8, N).astype(BF16)
    for o in NEAR_LAST:
        g_copy(o, tile).start()
    g_all[tile] = g_send[tile]
    halo_up.wait_recv()
    halo_down.wait_recv()
    lower = jnp.where(tile > 0, halo[0].astype(F32), 0.0)
    upper = jnp.where(tile < TILES - 1, halo[1].astype(F32), 0.0)
    for q in range(PEERS):
        here = vol_ref[:, q, :]
        before = lower if q == 0 else vol_ref[:, q - 1, :]
        after = upper if q == PEERS - 1 else vol_ref[:, q + 1, :]
        value = here - (tau_step * smooth_weight) * (2.0 * here - before - after)
        b_own[q] = value
        b_send[q] = value.astype(BF16)
    for p in range(PEERS):
        b_copy(p, mine).start()

    arrived(VOLUME)
    v_twin.start()
    arrived(COEF)
    coef_twin.start()

    def counted(rows, columns, dim):
        return lax.broadcasted_iota(jnp.int32, (rows, columns), dim)

    first_lane = counted(8, HALF, 1) == 0
    first_line = counted(8, N, 0) == 0
    lanes = counted(1, HALF, 1)
    freq_a = jnp.where(lanes == 0, HALF, lanes).astype(F32) * (1.0 / N)
    column_b = (counted(1, N, 1) - HALF).astype(F32) * (1.0 / N)

    def angle_tables(coefs, source, p):
        coef = coefs[source]
        step = coef[0:1, :] * freq_a
        sin_i, cos_i = sincos_turns(counted(8, HALF, 0).astype(F32) * step)
        sin_j, cos_j = sincos_turns((8 * counted(32, HALF, 0) - HALF).astype(F32) * step)
        for j in range(32):
            rows = slice(8 * j, 8 * j + 8)
            cos = cos_i * cos_j[j : j + 1] - sin_i * sin_j[j : j + 1]
            sin = sin_i * cos_j[j : j + 1] + cos_i * sin_j[j : j + 1]
            tab_a[p, 0, rows] = jnp.where(first_lane, 1.0, cos)
            tab_a[p, 1, rows] = jnp.where(first_lane, 0.0, sin)
            tab_a[p, 2, rows] = cos
        step = jnp.concatenate([coef[4:5, :], coef[4:5, :]], axis=1) * column_b
        sin_i, cos_i = sincos_turns(counted(8, N, 0).astype(F32) * step)
        sin_j, cos_j = sincos_turns((8 * counted(16, N, 0)).astype(F32) * step)
        unused, cos_end = sincos_turns(HALF * step)
        for j in range(16):
            rows = slice(8 * j, 8 * j + 8)
            cos = cos_i * cos_j[j : j + 1] - sin_i * sin_j[j : j + 1]
            sin = sin_i * cos_j[j : j + 1] + cos_i * sin_j[j : j + 1]
            tab_b[p, 0, rows] = cos
            tab_b[p, 1, rows] = sin
            tab_b[p, 2, rows] = jnp.where(first_line, cos_end, cos) if j == 0 else cos

    pl.loop(0, PEERS)(lambda p: angle_tables(coef_all, p, p))
    coef_twin.wait_recv()
    pl.loop(0, LATE)(lambda j: angle_tables(coef_other, 2 * ((x_me + 2 - j // 2) % 4) + j % 2, PEERS + j))

    def turned(p_part, q_part, table, p, rows, sign):
        cos, sin, end = table[p, 0, rows], table[p, 1, rows], table[p, 2, rows]
        if sign > 0:
            return p_part * cos + q_part * sin, q_part * end - p_part * sin
        return p_part * cos - q_part * sin, q_part * end + p_part * sin

    whole = slice(None)

    def sheared(place, js, prepare, start, middle, sign):
        for i, part in enumerate(parts):
            prepare(i, part)
            for j in js:
                for r in range(part.start, part.stop, STRIP):
                    rows = slice(r, r + STRIP)
                    first, second = start(j, rows)
                    first, second = turned(first, second, tab_a, place[j], rows, sign)
                    work_a[j, rows, :HALF] = first.astype(BF16)
                    work_a[j, rows, HALF:] = second.astype(BF16)
        middle()
        for j in js:
            work_b[j] = dot(work_a[j], tab_ref[INV_X]).astype(BF16)
        for j in js:
            y = dot(tab_ref[FWD_Y], work_b[j])
            first, second = turned(y[:HALF], y[HALF:], tab_b, place[j], whole, sign)
            work_a[j, :HALF] = first.astype(BF16)
            work_a[j, HALF:] = second.astype(BF16)
        for j in js:
            work_b[j] = dot(tab_ref[INV_Y], work_a[j]).astype(BF16)

    def projected(prepare, middle, groups, finish):
        sheared(order, range(PEERS), prepare, lambda j, rows: (xs[rows, :HALF], xs[rows, HALF:]), middle, 1)
        for js in groups:
            spectra = []
            for j in js:
                y = dot(work_b[j], tab_ref[FWD_X])
                turn = turned(y[:, :HALF], y[:, HALF:], tab_a, order[j], whole, 1)
                spectra.append(jnp.sum(jnp.concatenate(turn, axis=1), axis=0, keepdims=True))
            finish(js, spectra)

    def lines_of(spectra):
        return dot_parts(jnp.concatenate(spectra, axis=0), tab_ref[INV_X]) * (1.0 / math.sqrt(N))

    def nothing(*unused):
        pass

    copy(v_all.at[:, 1 - core], v_all.at[:, 1 - core], one_ss.at[0], one_rs.at[0], twin).wait_recv()
    xs[...] = dot(v_all[...].reshape(N, N), tab_ref[FWD_X])

    arrived(GRAD)
    grad = jnp.sum(g_all[...].astype(F32), axis=0)
    base = phase_ref[...] - eta_step * (grad + dual_ref[...] + rho_weight * phase_ref[...])
    lines = dot_parts(rho_weight * base + dual_ref[...], tab_ref[FWD_X])
    for q in range(PEERS):
        l_send[q] = lines[q : q + 1]
    for j, p in enumerate(order):
        l_copy(j, p, mine).start()

    def send_old(js, spectra):
        for j in js:
            old_send[j] = spectra[j - js[0]]
        for j in js:
            old_copy(j, order[j], my_slot).start()

    projected(nothing, nothing, [range(PEERS)], send_old)
    old_twin.start()

    arrived(SMOOTH)
    b_twin.start()

    def lines_in(group, rows):
        here = l_all.at[pl.ds(0, rows)]
        copy(here, here, sent.at[5], near_rs.at[group], twin).wait_recv()

    def backproject(place, js, asked, added):
        sheared(place, js, nothing, lambda j, rows: (asked[j][:, :HALF], asked[j][:, HALF:]), nothing, -1)
        for j in added:
            y = dot(work_b[j], tab_ref[FWD_X])
            turn = turned(y[:, :HALF], y[:, HALF:], tab_a, place[j], whole, -1)
            s_sum[...] += jnp.concatenate(turn, axis=1)

    def spectrum_asked(row_old, row_line):
        mine_part = (rho_weight * (1.0 - eta_step * rho_weight) / N) * old_send[row_old]
        return mine_part - (1.0 / math.sqrt(N)) * l_all[row_line]

    s_sum[...] = jnp.zeros((N, N), F32)

    @pl.when(core == 1)
    def _():
        for group, js in enumerate([(6, 7), (2, 3, 4, 5), (0, 1)]):
            lines_in(group, len(js))
            backproject(order, js, {j: spectrum_asked(j, order[j]) for j in js}, js)
        lines_in(3, LATE)

    @pl.when(core == 0)
    def _():
        lines_in(0, 2)
        lines_in(1, 2)

    old_twin.wait_recv()
    late = range(LATE)
    place = [jnp.where(core == 1, PEERS + j, order[LATE + j]) for j in late]
    asked = [
        spectrum_asked(LATE + j + core * (PEERS - LATE), jnp.where(core == 1, PEERS + order[j], order[LATE + j]))
        for j in late
    ]
    backproject(place, late, asked, late[:-1])
    last = LATE - 1
    for i, rows in enumerate(parts):
        y = dot(work_b[last, rows], tab_ref[FWD_X])
        turn = turned(y[:, :HALF], y[:, HALF:], tab_a, place[last], rows, -1)
        total = s_sum[rows] + jnp.concatenate(turn, axis=1)
        s_sum[rows] = total
        s_send[rows] = total.astype(BF16)
        s_twins[i].start()

    copy(b_all.at[:, 1 - core], b_all.at[:, 1 - core], one_ss.at[1], one_rs.at[1], twin).wait_recv()
    xb[...] = dot(b_all[...].reshape(N, N), tab_ref[FWD_X])

    def take_twin(i, rows):
        s_twins[i].wait_recv()
        total = s_sum[rows] + s_recv[rows].astype(F32)
        s_sum[rows] = total
        xs[rows] = xb[rows] - tau_step * total

    def send_back():
        blocks = s_sum[...].astype(BF16).reshape(PEERS, 2, ROWS, N)
        blocks = jnp.where(core == 0, blocks[:, 0], blocks[:, 1]).reshape(HALF, N)
        k_send[...] = dot(blocks, tab_ref[INV_X]).astype(BF16).reshape(PEERS, ROWS, N)
        for p in range(PEERS):
            k_copy(p, my_slot).start()

    def send_new(js, spectra):
        for j in js:
            new_send[j] = spectra[j - js[0]]
        for j in js:
            new_copy(j, order[j], my_slot).start()

    projected(take_twin, send_back, [range(2), range(2, 6), range(6, PEERS)], send_new)

    arrived(BACK)
    for q in range(PEERS):
        vol_out[:, q, :] = b_own[q] - tau_step * k_all[q].astype(F32)
    arrived(OLD)
    phase_new = base + (eta_step * rho_weight) * lines_of([old_all[q] for q in range(PEERS)])
    phase_out[...] = phase_new
    arrived(NEW)
    after = lines_of([new_all[q] for q in range(PEERS)])
    dual_out[...] = dual_ref[...] + rho_weight * (phase_new - after)

    for i, group in enumerate(groups):
        copy(group, group, sent.at[i], came.at[i], twin).wait_send()
    for one in [v_twin, b_twin, coef_twin, old_twin, halo_up, halo_down] + s_twins:
        one.wait_send()


def hand_over(phase_in, vol_in, dual_in, phase_out, vol_out, dual_out):
    phase_out[...] = phase_in[...]
    vol_out[...] = vol_in[...]
    dual_out[...] = dual_in[...]


def shards(volume, phase, dual, probe_real, probe_imag, intensity, offsets, angle_index):
    tables = jnp.asarray(packed_tables()).astype(BF16)
    in_vmem = pl.BlockSpec(memory_space=pltpu.VMEM)
    in_place = pl.BlockSpec(memory_space=pltpu.HBM)
    dma = pltpu.SemaphoreType.DMA
    vmem = pltpu.VMEM
    blocks = (PEERS, ROWS, N)
    lines = (PEERS, 1, N)
    results = (
        jax.ShapeDtypeStruct(phase.shape[1:], F32),
        jax.ShapeDtypeStruct(volume.shape, F32),
        jax.ShapeDtypeStruct(dual.shape[1:], F32),
    )
    made = pl.pallas_call(
        step_kernel,
        out_shape=results,
        in_specs=[in_place] * 9,
        out_specs=(in_vmem,) * 3,
        scratch_shapes=[
            pltpu.SMEM((1, SHOTS), jnp.int32),
            pltpu.SMEM((1,), jnp.int32),
            vmem(volume.shape, F32),
            vmem((8, N), F32),
            vmem((8, N), F32),
            vmem((HALF, HALF), F32),
            vmem((HALF, HALF), F32),
            vmem((SHOTS, HALF, HALF), F32),
            vmem(tables.shape, BF16),
            vmem((8, N), BF16),
            vmem((8, 128), F32),
            vmem((PEERS, 8, 128), F32),
            vmem((PEERS, 8, 128), F32),
            vmem(blocks, BF16),
            vmem((PEERS, 2, ROWS, N), BF16),
            vmem(blocks, BF16),
            vmem((PEERS, 2, ROWS, N), BF16),
            vmem(blocks, F32),
            vmem((2, ROWS, N), BF16),
            vmem((TILES, 8, N), BF16),
            vmem((TILES, 8, N), BF16),
            vmem((TILES, 8, N), BF16),
            vmem(lines, F32),
            vmem((2 * PEERS, 1, N), F32),
            vmem((2 * PEERS, 1, N), F32),
            vmem(lines, F32),
            vmem(lines, F32),
            vmem(lines, F32),
            vmem(blocks, BF16),
            vmem(blocks, BF16),
            vmem((N, N), BF16),
            vmem((N, N), BF16),
            vmem((PEERS, N, N), BF16),
            vmem((PEERS, N, N), BF16),
            vmem(volume.shape, F32),
            vmem((8, N), F32),
            vmem((8, N), F32),
            vmem((PEERS + LATE, 3, N, HALF), F32),
            vmem((PEERS + LATE, 3, HALF, N), F32),
            vmem((N, N), F32),
            vmem((N, N), F32),
            vmem((N, N), F32),
            vmem((SHOTS, 2, HALF, HALF), F32),
            dma((9,)),
            dma((9,)),
            dma((4,)),
            dma((6,)),
            dma((6,)),
            dma((PARTS,)),
            dma((PARTS,)),
            dma((9,)),
        ],
        compiler_params=pltpu.CompilerParams(collective_id=0, has_side_effects=True, vmem_limit_bytes=24 << 20),
    )(*[pltpu.with_memory_space_constraint(x, pltpu.HBM) for x in (offsets,)], angle_index, *[pltpu.with_memory_space_constraint(x, pltpu.HBM) for x in (volume, phase[0], dual[0], probe_real, probe_imag, intensity[0], tables)])
    phase_new, volume_new, dual_new = pl.pallas_call(
        hand_over, out_shape=results, in_specs=[in_vmem] * 3, out_specs=(in_vmem,) * 3, compiler_params=pltpu.CompilerParams(vmem_limit_bytes=4 << 20)
    )(*made)
    return (phase_new[None], volume_new, dual_new[None])


def solution(mesh):
    placed = (
        P("ang", "tile", None),
        P("ang", "tile", None),
        P("ang", "tile", None),
        P(),
        P(),
        P("ang", "tile", None, None),
        P("ang", "tile"),
        P("ang"),
    )
    return jax.shard_map(
        shards,
        mesh=mesh,
        in_specs=placed,
        out_specs=(P("ang", "tile", None), P("ang", "tile", None), P("ang", "tile", None)),
        check_vma=False,
    )
```

```python
import math

import jax
import jax.numpy as jnp
import numpy as np
from jax import lax
from jax.experimental import pallas as pl
from jax.experimental.pallas import tpu as pltpu
from jax.sharding import PartitionSpec as P

angle_center = 90.0
rho_weight = 1.0
eta_step = 0.01
tau_step = 1.0
smooth_weight = 0.25

N = 256
HALF = 128
PEERS = 8
TILES = 16
ROWS = 16
SHOTS = 4
BAND_ROWS = 128
STRIP = 32
FWD_X, INV_X, FWD_Y, INV_Y = range(4)
PHASE, GRAD, COEF, VOLUME, SMOOTH, LINES, OLD, NEW, BACK = range(9)
PARTS = 2
AWAY = [2, 2, 1, 1, 1, 1, 0, 0]
MOVED = (0, 1, 4, 5)
LATE = 4
NEAR_LAST = [4 * dy + dz for dy in (2, 1, 3, 0) for dz in range(4) if dy or dz]
F32 = jnp.float32
BF16 = jnp.bfloat16
MESH = pl.DeviceIdType.MESH


def tables_of(length):
    index = np.arange(length)
    phases = (index[:, None] * index[None, :] % length).astype(np.float32)
    phases = phases * np.float32(2.0 * math.pi / length)
    return np.cos(phases), np.sin(phases)


def packed_tables():
    cos, sin = tables_of(N)
    signs = np.where(np.arange(N) % 2 == 0, 1.0, -1.0)
    forward = np.concatenate([cos[:, :HALF], -sin[:, :HALF]], axis=1)
    forward[:, HALF] = signs
    inverse = np.concatenate([2.0 * cos[:HALF], -2.0 * sin[:HALF]], axis=0)
    inverse[0] = 1.0
    inverse[HALF] = signs
    inverse = inverse / N
    cos, sin = tables_of(HALF)
    cos, sin = cos / math.sqrt(HALF), sin / math.sqrt(HALF)
    near = np.block([[cos, -sin], [sin, cos]])
    away = np.block([[cos, sin], [-sin, cos]])
    stack = np.stack([forward, inverse, forward.T, inverse.T, near, away])
    return stack.astype(np.float32)


def sincos_turns(turns):
    a = (turns - jnp.floor(turns + 0.5)) * math.pi
    z = a * a
    sin = 1.0
    for k in (12, 10, 8, 6, 4, 2):
        sin = 1.0 - z * sin * (1.0 / (k * (k + 1)))
    sin = a * sin
    cos = 1.0
    for k in (13, 11, 9, 7, 5, 3, 1):
        cos = 1.0 - z * cos * (1.0 / (k * (k + 1)))
    return 2.0 * sin * cos, 1.0 - 2.0 * sin * sin


def dot(a, b):
    return jnp.dot(a, b, preferred_element_type=F32)


def two_parts(x):
    high = x.astype(BF16)
    low = (x - high.astype(F32)).astype(BF16)
    return jnp.concatenate([high, low], axis=0)


def dot_parts(x, table):
    both = dot(two_parts(x), table)
    return both[: x.shape[0]] + both[x.shape[0] :]


def step_kernel(
    offsets_in, angle_in, vol_in, phase_in, dual_in, pr_in, pi_in, inten_in, tab_in,
    phase_out, vol_out, dual_out,
    offsets_ref, angle_ref, vol_ref, phase_ref, dual_ref, pr_ref, pi_ref, inten_ref, tab_ref, phase_send,
    coef_send, coef_all, coef_other, v_send, v_all, b_send, b_all, b_own, halo, phase_all, g_send, g_all, l_send, l_all,
    old_send, old_all, new_send, new_all, k_send, k_all, s_send, s_recv,
    work_a, work_b, vol_made, phase_made, dual_made, tab_a, tab_b, xs, xb, s_sum, wave,
    sent, came, near_rs, one_ss, one_rs, part_ss, part_rs, in_sem,
):
    me = lax.axis_index("ang")
    tile = lax.axis_index("tile")
    core = me % 2
    mine = me // 2
    x_me, hi_me = mine // 2, mine % 2
    low = tile % 4
    far_tile = (tile // 4) * 4 + (low + 2) % 4
    turn_out = (low + 2) // 4
    turn_in = ((low + 2) % 4 + 2) // 4
    my_slot = 2 * x_me + (hi_me + turn_in) % 2
    twin = (me - core + (1 - core), tile)

    def peer(p):
        return (2 * p + core, far_tile)

    def slot_of(p):
        return 2 * (p // 2) + (p % 2 + turn_out) % 2

    def beside(o):
        return (me, ((tile // 4 + o // 4) % 4) * 4 + (low + o) % 4)

    order = [2 * ((x_me + dx) % 4) + zh for dx in (2, 1, 3, 0) for zh in (0, 1)]

    barrier = pltpu.get_barrier_semaphore()
    for o in NEAR_LAST:
        pl.semaphore_signal(barrier, inc=1, device_id=beside(o), device_id_type=MESH)
    for p in range(PEERS):
        pl.semaphore_signal(barrier, inc=1, device_id=peer(p), device_id_type=MESH)
    for p in range(PEERS):
        pl.semaphore_signal(barrier, inc=1, device_id=(2 * p + 1 - core, far_tile), device_id_type=MESH)
    pl.semaphore_signal(barrier, inc=1, device_id=twin, device_id_type=MESH)

    loads = [
        pltpu.make_async_copy(src, dst, in_sem.at[i])
        for i, (src, dst) in enumerate(
            [
                (angle_in, angle_ref), (phase_in, phase_ref), (vol_in, vol_ref), (offsets_in, offsets_ref),
                (pr_in, pr_ref), (pi_in, pi_ref), (inten_in, inten_ref), (tab_in, tab_ref), (dual_in, dual_ref),
            ]
        )
    ]
    for load in loads:
        load.start()

    loads[0].wait()
    number = jnp.full((8, 128), angle_ref[0], jnp.int32).astype(F32) - angle_center
    sin_b, unused = sincos_turns(number * (1.0 / 720.0))
    sin_h, cos_h = sincos_turns(number * (1.0 / 1440.0))
    rows8 = lax.broadcasted_iota(jnp.int32, (8, 128), 0)
    coef_send[...] = jnp.where(rows8 < 4, -(sin_h / cos_h), sin_b)
    loads[1].wait()
    turns = phase_ref[...] * (1.0 / (2.0 * math.pi))
    phase_send[...] = (turns - jnp.floor(turns + 0.5)).astype(BF16)
    loads[2].wait()
    for q in range(PEERS):
        v_send[q] = vol_ref[:, q, :].astype(BF16)

    pl.semaphore_wait(barrier, TILES + 2 * PEERS)

    def copy(src, dst, send, recv, device):
        return pltpu.make_async_remote_copy(
            src_ref=src, dst_ref=dst, send_sem=send, recv_sem=recv, device_id=device, device_id_type=MESH
        )

    def phase_copy(o, slot):
        return copy(phase_send, phase_all.at[slot], sent.at[0], came.at[0], beside(o))

    def coef_copy(p, slot):
        return copy(coef_send, coef_all.at[slot], sent.at[2], came.at[2], peer(p))

    def v_copy(p, slot):
        return copy(v_send.at[slot_of(p)], v_all.at[slot, core], sent.at[3], came.at[3], peer(p))

    def b_copy(p, slot):
        return copy(b_send.at[slot_of(p)], b_all.at[slot, core], sent.at[4], came.at[4], peer(p))

    def g_copy(o, slot):
        return copy(g_send.at[beside(o)[1]], g_all.at[slot], sent.at[1], came.at[1], beside(o))

    def l_copy(j, p, slot):
        if j in MOVED:
            row, came_at = slot + PEERS * (1 - core), jnp.where(core == 1, AWAY[j], 3)
            return copy(l_send.at[slot_of(p)], l_all.at[row], sent.at[5], near_rs.at[came_at], (2 * p + 1, far_tile))
        return copy(l_send.at[slot_of(p)], l_all.at[slot], sent.at[5], near_rs.at[AWAY[j]], peer(p))

    def old_copy(j, p, slot):
        return copy(old_send.at[j], old_all.at[slot], sent.at[6], came.at[6], peer(p))

    def new_copy(j, p, slot):
        return copy(new_send.at[j], new_all.at[slot], sent.at[7], came.at[7], peer(p))

    def k_copy(p, slot):
        return copy(k_send.at[p], k_all.at[slot], sent.at[8], came.at[8], peer(p))

    others = pl.ds(0, TILES - 1)
    groups = [phase_all.at[others], g_all.at[others], coef_all, v_send, b_send, l_send, old_all, new_send, k_send]

    def arrived(group):
        copy(groups[group], groups[group], sent.at[group], came.at[group], twin).wait_recv()

    v_twin = copy(v_all.at[:, core], v_all.at[:, core], one_ss.at[0], one_rs.at[0], twin)
    b_twin = copy(b_all.at[:, core], b_all.at[:, core], one_ss.at[1], one_rs.at[1], twin)
    parts = [slice(r, r + N // PARTS) for r in range(0, N, N // PARTS)]
    s_twins = [
        copy(s_send.at[rows], s_recv.at[rows], part_ss.at[i], part_rs.at[i], twin) for i, rows in enumerate(parts)
    ]
    coef_twin = copy(coef_all, coef_other, one_ss.at[4], one_rs.at[4], twin)
    old_twin = copy(old_send.at[pl.ds(0, PEERS)], old_send.at[pl.ds(PEERS, PEERS)], one_ss.at[5], one_rs.at[5], twin)
    halo_up = copy(v_send.at[PEERS - 1], halo.at[0], one_ss.at[2], one_rs.at[2], (me, (tile + 1) % TILES))
    halo_down = copy(v_send.at[0], halo.at[1], one_ss.at[3], one_rs.at[3], (me, (tile + TILES - 1) % TILES))

    for o in NEAR_LAST:
        phase_copy(o, tile).start()
    for p in range(PEERS):
        coef_copy(p, mine).start()
    for p in range(PEERS):
        v_copy(p, mine).start()
    halo_up.start()
    halo_down.start()
    phase_all[tile] = phase_send[...]
    for load in loads[3:]:
        load.wait()
    near, away = tab_ref[4], tab_ref[5]

    arrived(PHASE)

    sin, cos = sincos_turns(phase_all[...].astype(F32).reshape(BAND_ROWS, N))
    column = lax.broadcasted_iota(jnp.int32, (BAND_ROWS, HALF), 1)
    waves = []
    for s in range(SHOTS):
        back = (N - offsets_ref[0, s]) % HALF
        from_left = column >= offsets_ref[0, s]
        c = pltpu.roll(jnp.where(from_left, cos[:, :HALF], cos[:, HALF:]), back, 1)
        n = pltpu.roll(jnp.where(from_left, sin[:, :HALF], sin[:, HALF:]), back, 1)
        wave_r = pr_ref[...] * c - pi_ref[...] * n
        wave_i = pr_ref[...] * n + pi_ref[...] * c
        wave[s, 0] = wave_r
        wave[s, 1] = wave_i
        waves.append(jnp.concatenate([wave_r, wave_i], axis=1).astype(BF16))
    half = dot(jnp.concatenate(waves, axis=0), near).astype(BF16)
    beams = [half[s * HALF : (s + 1) * HALF] for s in range(SHOTS)]
    beams = [jnp.concatenate([b[:, :HALF], b[:, HALF:]], axis=0) for b in beams]
    far = dot(away, jnp.concatenate(beams, axis=1))
    far_r, far_i = far[:HALF], far[HALF:]
    measured = jnp.concatenate([inten_ref[s] for s in range(SHOTS)], axis=1)
    misfit = far_r * far_r + far_i * far_i - measured
    weighted = jnp.concatenate([misfit * far_r, misfit * far_i], axis=0).astype(BF16)
    half = dot(near, weighted).astype(BF16)
    beams = [half[:, s * HALF : (s + 1) * HALF] for s in range(SHOTS)]
    beams = [jnp.concatenate([b[:HALF], b[HALF:]], axis=1) for b in beams]
    leave = dot(jnp.concatenate(beams, axis=0), away)
    image = jnp.zeros((BAND_ROWS, N), F32)
    for s in range(SHOTS):
        e = leave[s * HALF : (s + 1) * HALF]
        term = 2.0 * (e[:, HALF:] * wave[s, 0] - e[:, :HALF] * wave[s, 1])
        term = pltpu.roll(term, offsets_ref[0, s] % HALF, 1)
        in_left = column >= offsets_ref[0, s]
        image = image + jnp.concatenate([jnp.where(in_left, term, 0.0), jnp.where(in_left, 0.0, term)], axis=1)
    g_send[...] = image.reshape(TILES, 8, N).astype(BF16)
    for o in NEAR_LAST:
        g_copy(o, tile).start()
    g_all[tile] = g_send[tile]
    halo_up.wait_recv()
    halo_down.wait_recv()
    lower = jnp.where(tile > 0, halo[0].astype(F32), 0.0)
    upper = jnp.where(tile < TILES - 1, halo[1].astype(F32), 0.0)
    for q in range(PEERS):
        here = vol_ref[:, q, :]
        before = lower if q == 0 else vol_ref[:, q - 1, :]
        after = upper if q == PEERS - 1 else vol_ref[:, q + 1, :]
        value = here - (tau_step * smooth_weight) * (2.0 * here - before - after)
        b_own[q] = value
        b_send[q] = value.astype(BF16)
    for p in range(PEERS):
        b_copy(p, mine).start()

    arrived(VOLUME)
    v_twin.start()
    arrived(COEF)
    coef_twin.start()

    def counted(rows, columns, dim):
        return lax.broadcasted_iota(jnp.int32, (rows, columns), dim)

    first_lane = counted(8, HALF, 1) == 0
    first_line = counted(8, N, 0) == 0
    lanes = counted(1, HALF, 1)
    freq_a = jnp.where(lanes == 0, HALF, lanes).astype(F32) * (1.0 / N)
    column_b = (counted(1, N, 1) - HALF).astype(F32) * (1.0 / N)

    def angle_tables(coefs, source, p):
        coef = coefs[source]
        step = coef[0:1, :] * freq_a
        sin_i, cos_i = sincos_turns(counted(8, HALF, 0).astype(F32) * step)
        sin_j, cos_j = sincos_turns((8 * counted(32, HALF, 0) - HALF).astype(F32) * step)
        for j in range(32):
            rows = slice(8 * j, 8 * j + 8)
            cos = cos_i * cos_j[j : j + 1] - sin_i * sin_j[j : j + 1]
            sin = sin_i * cos_j[j : j + 1] + cos_i * sin_j[j : j + 1]
            tab_a[p, 0, rows] = jnp.where(first_lane, 1.0, cos)
            tab_a[p, 1, rows] = jnp.where(first_lane, 0.0, sin)
            tab_a[p, 2, rows] = cos
        step = jnp.concatenate([coef[4:5, :], coef[4:5, :]], axis=1) * column_b
        sin_i, cos_i = sincos_turns(counted(8, N, 0).astype(F32) * step)
        sin_j, cos_j = sincos_turns((8 * counted(16, N, 0)).astype(F32) * step)
        unused, cos_end = sincos_turns(HALF * step)
        for j in range(16):
            rows = slice(8 * j, 8 * j + 8)
            cos = cos_i * cos_j[j : j + 1] - sin_i * sin_j[j : j + 1]
            sin = sin_i * cos_j[j : j + 1] + cos_i * sin_j[j : j + 1]
            tab_b[p, 0, rows] = cos
            tab_b[p, 1, rows] = sin
            tab_b[p, 2, rows] = jnp.where(first_line, cos_end, cos) if j == 0 else cos

    pl.loop(0, PEERS)(lambda p: angle_tables(coef_all, p, p))
    coef_twin.wait_recv()
    pl.loop(0, LATE)(lambda j: angle_tables(coef_other, 2 * ((x_me + 2 - j // 2) % 4) + j % 2, PEERS + j))

    def turned(p_part, q_part, table, p, rows, sign):
        cos, sin, end = table[p, 0, rows], table[p, 1, rows], table[p, 2, rows]
        if sign > 0:
            return p_part * cos + q_part * sin, q_part * end - p_part * sin
        return p_part * cos - q_part * sin, q_part * end + p_part * sin

    whole = slice(None)

    def sheared(place, js, prepare, start, middle, sign):
        for i, part in enumerate(parts):
            prepare(i, part)
            for j in js:
                for r in range(part.start, part.stop, STRIP):
                    rows = slice(r, r + STRIP)
                    first, second = start(j, rows)
                    first, second = turned(first, second, tab_a, place[j], rows, sign)
                    work_a[j, rows, :HALF] = first.astype(BF16)
                    work_a[j, rows, HALF:] = second.astype(BF16)
        middle()
        for j in js:
            work_b[j] = dot(work_a[j], tab_ref[INV_X]).astype(BF16)
        for j in js:
            y = dot(tab_ref[FWD_Y], work_b[j])
            first, second = turned(y[:HALF], y[HALF:], tab_b, place[j], whole, sign)
            work_a[j, :HALF] = first.astype(BF16)
            work_a[j, HALF:] = second.astype(BF16)
        for j in js:
            work_b[j] = dot(tab_ref[INV_Y], work_a[j]).astype(BF16)

    def projected(prepare, middle, groups, finish):
        sheared(order, range(PEERS), prepare, lambda j, rows: (xs[rows, :HALF], xs[rows, HALF:]), middle, 1)
        for js in groups:
            spectra = []
            for j in js:
                y = dot(work_b[j], tab_ref[FWD_X])
                turn = turned(y[:, :HALF], y[:, HALF:], tab_a, order[j], whole, 1)
                spectra.append(jnp.sum(jnp.concatenate(turn, axis=1), axis=0, keepdims=True))
            finish(js, spectra)

    def lines_of(spectra):
        return dot_parts(jnp.concatenate(spectra, axis=0), tab_ref[INV_X]) * (1.0 / math.sqrt(N))

    def nothing(*unused):
        pass

    copy(v_all.at[:, 1 - core], v_all.at[:, 1 - core], one_ss.at[0], one_rs.at[0], twin).wait_recv()
    xs[...] = dot(v_all[...].reshape(N, N), tab_ref[FWD_X])

    arrived(GRAD)
    grad = jnp.sum(g_all[...].astype(F32), axis=0)
    base = phase_ref[...] - eta_step * (grad + dual_ref[...] + rho_weight * phase_ref[...])
    lines = dot_parts(rho_weight * base + dual_ref[...], tab_ref[FWD_X])
    for q in range(PEERS):
        l_send[q] = lines[q : q + 1]
    for j, p in enumerate(order):
        l_copy(j, p, mine).start()

    def send_old(js, spectra):
        for j in js:
            old_send[j] = spectra[j - js[0]]
        for j in js:
            old_copy(j, order[j], my_slot).start()

    projected(nothing, nothing, [range(PEERS)], send_old)
    old_twin.start()

    arrived(SMOOTH)
    b_twin.start()

    def lines_in(group, rows):
        here = l_all.at[pl.ds(0, rows)]
        copy(here, here, sent.at[5], near_rs.at[group], twin).wait_recv()

    def backproject(place, js, asked, added):
        sheared(place, js, nothing, lambda j, rows: (asked[j][:, :HALF], asked[j][:, HALF:]), nothing, -1)
        for j in added:
            y = dot(work_b[j], tab_ref[FWD_X])
            turn = turned(y[:, :HALF], y[:, HALF:], tab_a, place[j], whole, -1)
            s_sum[...] += jnp.concatenate(turn, axis=1)

    def spectrum_asked(row_old, row_line):
        mine_part = (rho_weight * (1.0 - eta_step * rho_weight) / N) * old_send[row_old]
        return mine_part - (1.0 / math.sqrt(N)) * l_all[row_line]

    s_sum[...] = jnp.zeros((N, N), F32)

    @pl.when(core == 1)
    def _():
        for group, js in enumerate([(6, 7), (2, 3, 4, 5), (0, 1)]):
            lines_in(group, len(js))
            backproject(order, js, {j: spectrum_asked(j, order[j]) for j in js}, js)
        lines_in(3, LATE)

    @pl.when(core == 0)
    def _():
        lines_in(0, 2)
        lines_in(1, 2)

    old_twin.wait_recv()
    late = range(LATE)
    place = [jnp.where(core == 1, PEERS + j, order[LATE + j]) for j in late]
    asked = [
        spectrum_asked(LATE + j + core * (PEERS - LATE), jnp.where(core == 1, PEERS + order[j], order[LATE + j]))
        for j in late
    ]
    backproject(place, late, asked, late[:-1])
    last = LATE - 1
    for i, rows in enumerate(parts):
        y = dot(work_b[last, rows], tab_ref[FWD_X])
        turn = turned(y[:, :HALF], y[:, HALF:], tab_a, place[last], rows, -1)
        total = s_sum[rows] + jnp.concatenate(turn, axis=1)
        s_sum[rows] = total
        s_send[rows] = total.astype(BF16)
        s_twins[i].start()

    copy(b_all.at[:, 1 - core], b_all.at[:, 1 - core], one_ss.at[1], one_rs.at[1], twin).wait_recv()
    xb[...] = dot(b_all[...].reshape(N, N), tab_ref[FWD_X])

    def take_twin(i, rows):
        s_twins[i].wait_recv()
        total = s_sum[rows] + s_recv[rows].astype(F32)
        s_sum[rows] = total
        xs[rows] = xb[rows] - tau_step * total

    def send_back():
        blocks = s_sum[...].astype(BF16).reshape(PEERS, 2, ROWS, N)
        blocks = jnp.where(core == 0, blocks[:, 0], blocks[:, 1]).reshape(HALF, N)
        k_send[...] = dot(blocks, tab_ref[INV_X]).astype(BF16).reshape(PEERS, ROWS, N)
        for p in range(PEERS):
            k_copy(p, my_slot).start()

    def send_new(js, spectra):
        for j in js:
            new_send[j] = spectra[j - js[0]]
        for j in js:
            new_copy(j, order[j], my_slot).start()

    projected(take_twin, send_back, [range(2), range(2, 6), range(6, PEERS)], send_new)

    arrived(BACK)
    for q in range(PEERS):
        vol_out[:, q, :] = b_own[q] - tau_step * k_all[q].astype(F32)
    arrived(OLD)
    phase_new = base + (eta_step * rho_weight) * lines_of([old_all[q] for q in range(PEERS)])
    phase_out[...] = phase_new
    arrived(NEW)
    after = lines_of([new_all[q] for q in range(PEERS)])
    dual_out[...] = dual_ref[...] + rho_weight * (phase_new - after)

    for i, group in enumerate(groups):
        copy(group, group, sent.at[i], came.at[i], twin).wait_send()
    for one in [v_twin, b_twin, coef_twin, old_twin, halo_up, halo_down] + s_twins:
        one.wait_send()


def hand_over(phase_in, vol_in, dual_in, phase_out, vol_out, dual_out):
    phase_out[...] = phase_in[...]
    vol_out[...] = vol_in[...]
    dual_out[...] = dual_in[...]


def shards(volume, phase, dual, probe_real, probe_imag, intensity, offsets, angle_index):
    tables = jnp.asarray(packed_tables()).astype(BF16)
    in_vmem = pl.BlockSpec(memory_space=pltpu.VMEM)
    in_place = pl.BlockSpec(memory_space=pltpu.HBM)
    dma = pltpu.SemaphoreType.DMA
    vmem = pltpu.VMEM
    blocks = (PEERS, ROWS, N)
    lines = (PEERS, 1, N)
    results = (
        jax.ShapeDtypeStruct(phase.shape[1:], F32),
        jax.ShapeDtypeStruct(volume.shape, F32),
        jax.ShapeDtypeStruct(dual.shape[1:], F32),
    )
    made = pl.pallas_call(
        step_kernel,
        out_shape=results,
        in_specs=[in_place] * 9,
        out_specs=(in_vmem,) * 3,
        scratch_shapes=[
            pltpu.SMEM((1, SHOTS), jnp.int32),
            pltpu.SMEM((1,), jnp.int32),
            vmem(volume.shape, F32),
            vmem((8, N), F32),
            vmem((8, N), F32),
            vmem((HALF, HALF), F32),
            vmem((HALF, HALF), F32),
            vmem((SHOTS, HALF, HALF), F32),
            vmem(tables.shape, BF16),
            vmem((8, N), BF16),
            vmem((8, 128), F32),
            vmem((PEERS, 8, 128), F32),
            vmem((PEERS, 8, 128), F32),
            vmem(blocks, BF16),
            vmem((PEERS, 2, ROWS, N), BF16),
            vmem(blocks, BF16),
            vmem((PEERS, 2, ROWS, N), BF16),
            vmem(blocks, F32),
            vmem((2, ROWS, N), BF16),
            vmem((TILES, 8, N), BF16),
            vmem((TILES, 8, N), BF16),
            vmem((TILES, 8, N), BF16),
            vmem(lines, F32),
            vmem((2 * PEERS, 1, N), F32),
            vmem((2 * PEERS, 1, N), F32),
            vmem(lines, F32),
            vmem(lines, F32),
            vmem(lines, F32),
            vmem(blocks, BF16),
            vmem(blocks, BF16),
            vmem((N, N), BF16),
            vmem((N, N), BF16),
            vmem((PEERS, N, N), BF16),
            vmem((PEERS, N, N), BF16),
            vmem(volume.shape, F32),
            vmem((8, N), F32),
            vmem((8, N), F32),
            vmem((PEERS + LATE, 3, N, HALF), F32),
            vmem((PEERS + LATE, 3, HALF, N), F32),
            vmem((N, N), F32),
            vmem((N, N), F32),
            vmem((N, N), F32),
            vmem((SHOTS, 2, HALF, HALF), F32),
            dma((9,)),
            dma((9,)),
            dma((4,)),
            dma((6,)),
            dma((6,)),
            dma((PARTS,)),
            dma((PARTS,)),
            dma((9,)),
        ],
        compiler_params=pltpu.CompilerParams(collective_id=0, has_side_effects=True, vmem_limit_bytes=24 << 20),
    )(*[pltpu.with_memory_space_constraint(x, pltpu.HBM) for x in (offsets,)], angle_index, *[pltpu.with_memory_space_constraint(x, pltpu.HBM) for x in (volume, phase[0], dual[0], probe_real, probe_imag, intensity[0], tables)])
    phase_new, volume_new, dual_new = pl.pallas_call(
        hand_over, out_shape=results, in_specs=[in_vmem] * 3, out_specs=(in_vmem,) * 3, compiler_params=pltpu.CompilerParams(vmem_limit_bytes=4 << 20)
    )(*made)
    return (phase_new[None], volume_new, dual_new[None])


def solution(mesh):
    placed = (
        P("ang", "tile", None),
        P("ang", "tile", None),
        P("ang", "tile", None),
        P(),
        P(),
        P("ang", "tile", None, None),
        P("ang", "tile"),
        P("ang"),
    )
    return jax.shard_map(
        shards,
        mesh=mesh,
        in_specs=placed,
        out_specs=(P("ang", "tile", None), P("ang", "tile", None), P("ang", "tile", None)),
        check_vma=False,
    )
```
